32 devices in a mesh: vocab: 8 (over z, x), tok: 4 (over y, core).
Axes of the slice: x: 2, y: 2, z: 4, core: 2. Of those that a mesh axis runs over, the one named last changes fastest.
Arguments:
- hidden: bfloat16 [768, 7168], P('tok', 'vocab'), may hold values from -21 to 21
- head_weight: bfloat16 [7168, 8192], P('tok', 'vocab'), may hold values from -0.12695312 to 0.12695312
- targets: int32 [768], P('tok'), may hold values from 0 to 6143
- vocab_mask: int32 [8192], P('vocab'), may hold values from 0 to 1, as said below
- token_grad: float32 [768], P('tok'), may hold values from 16 to 160
Outputs:
- hidden_grad: bfloat16 [768, 7168], P('tok', 'vocab')
- token_loss: float32 [768], P('tok')
The draws below stay inside these ranges and needn't reach their ends.
Inputs may be any that keep to these rules, and one draw needn't show every extreme that they name: vocab_mask is 1 on the columns below some cut and 0 from it on, with between 1 and 2048 zeros.
All inputs are finite; a program needn't handle non-finite values.
Results may differ from the reference program's by a relative error of at most 0.0051.
Values may be sent and summed in bfloat16 or wider, within the bound.
A program may use at most 64 MiB of HBM per device.

```python
import math
import jax
import jax.numpy as jnp
from jax import lax

D = 7168
V = 8192
TOKENS = 768


def draw_head_weight(key, part):
    weights = jnp.clip(jax.random.normal(jax.random.fold_in(key, 11), (D, V), jnp.float32), -6.0, 6.0) * D ** (-0.5)
    return weights.astype(jnp.bfloat16)


def draw_hidden(key, part):
    values = 3.0 * jnp.clip(jax.random.normal(jax.random.fold_in(key, 23), (TOKENS, D), jnp.float32), -6.0, 6.0)
    return values.astype(jnp.bfloat16)


def draw_vocab_mask(key, part):
    padding = jax.random.randint(jax.random.fold_in(key, 31), (), 1, V // 4 + 1)
    return (jnp.arange(V, dtype=jnp.int32) < V - padding).astype(jnp.int32)


def with_ends(values, own_key, low, high):
    spot = [jax.random.randint(jax.random.fold_in(own_key, axis), (), 0, length) for axis, length in enumerate(values.shape)]
    widest = values.shape.index(max(values.shape))
    next_to = spot[:widest] + [(spot[widest] + 1) % values.shape[widest]] + spot[widest + 1:]
    return values.at[tuple(spot)].set(low).at[tuple(next_to)].set(high)


def steps_of(stream_key, dims, shards, least, top_value):
    def one(position, shards_of):
        heights = jax.random.uniform(jax.random.fold_in(jax.random.fold_in(stream_key, 6), position), (shards_of,), jnp.float32, least / len(shards), top_value / len(shards))
        return jnp.repeat(jnp.exp(heights), dims[position] // shards_of).reshape((-1,) + (1,) * (len(dims) - position - 1))

    factor_of = one(*shards[0])
    for cut in shards[1:]:
        factor_of = factor_of * one(*cut)
    return factor_of


def setup_inputs(seed: int = 0) -> dict:
    keys = jax.random.split(jax.random.key(seed), 6)
    hidden = draw_hidden(jax.random.fold_in(keys[5], 71), 0)
    head_weight = draw_head_weight(jax.random.fold_in(keys[5], 71), 0)
    targets = with_ends(jax.random.randint(keys[2], (TOKENS,), 0, 3 * V // 4), jax.random.fold_in(keys[2], 1), 0, (3 * V // 4) - 1).astype(jnp.int32)
    vocab_mask = draw_vocab_mask(jax.random.fold_in(keys[5], 71), 0)
    token_grad = jnp.clip(jnp.exp(math.log(160.0) - 2.3025851 * jax.random.uniform(keys[4], (TOKENS,), jnp.float32) ** steps_of(keys[4], (TOKENS,), ((0, 4),), -0.2, 0.2)), 16.0, 160.0)
    return dict(hidden=hidden, head_weight=head_weight, targets=targets, vocab_mask=vocab_mask, token_grad=token_grad)


def reference(hidden, head_weight, targets, vocab_mask, token_grad):
    logits = jnp.dot(hidden, head_weight, preferred_element_type=jnp.float32)
    live_mask = vocab_mask[None, :] == 1
    masked = jnp.where(live_mask, logits, jnp.float32(-1e30))
    row_max = jnp.max(masked, axis=1)
    denominator = jnp.sum(jnp.exp(masked - row_max[:, None]), axis=1)
    columns = jnp.arange(V, dtype=jnp.int32)
    onehot = columns[None, :] == targets[:, None].astype(jnp.int32)
    target_logit = jnp.sum(jnp.where(onehot, logits, jnp.float32(0.0)), axis=1)
    log_norm = row_max + jnp.log(denominator)
    token_loss = log_norm - target_logit
    probabilities = jnp.exp(masked - log_norm[:, None])
    logit_grad = (token_grad[:, None] * (probabilities - onehot.astype(jnp.float32))).astype(jnp.bfloat16)
    hidden_grad = lax.dot_general(logit_grad, head_weight, (((1,), (1,)), ((), ())), preferred_element_type=jnp.float32)
    return hidden_grad.astype(jnp.bfloat16), token_loss
```

```python
import jax
import jax.numpy as jnp
from jax import lax
from jax.experimental import pallas as pl
from jax.experimental.pallas import tpu as pltpu
from jax.sharding import PartitionSpec as P


def make_on_device(vocab_size, tok_size):
    share = vocab_size // tok_size
    moves = [
        (b * tok_size + a, (a * share + b % share) * tok_size + b // share)
        for a in range(tok_size)
        for b in range(vocab_size)
    ]
    back = [(there, here) for here, there in moves]

    def on_device(hidden, head_weight, targets, vocab_mask, token_grad):
        rows, feats = hidden.shape
        block_width = head_weight.shape[1]
        moved = lax.ppermute(hidden, ("vocab", "tok"), moves)
        pieces = lax.all_gather(moved, "vocab")
        gathered = (
            pieces.reshape(tok_size, share, rows, feats)
            .transpose(0, 2, 1, 3)
            .reshape(tok_size * rows, share * feats)
        )
        partial_logits = jnp.dot(gathered, head_weight, preferred_element_type=jnp.float32)
        logits = lax.psum_scatter(partial_logits, "tok", scatter_dimension=0, tiled=True)
        first_column = lax.axis_index("vocab") * block_width
        masked = jnp.where(vocab_mask[None, :] == 1, logits, jnp.float32(-1e30))
        local_max = jnp.max(masked, axis=1)
        columns = first_column + jnp.arange(block_width, dtype=jnp.int32)
        onehot = columns[None, :] == targets[:, None]
        local_target = jnp.sum(jnp.where(onehot, logits, jnp.float32(0.0)), axis=1)
        weights = jnp.exp(masked - local_max[:, None])
        local_sum = jnp.sum(weights, axis=1)
        stats = lax.all_gather(jnp.stack([local_max, local_sum, local_target]), "vocab")
        row_max = jnp.max(stats[:, 0], axis=0)
        denominator = jnp.sum(stats[:, 1] * jnp.exp(stats[:, 0] - row_max[None]), axis=0)
        target_logit = jnp.sum(stats[:, 2], axis=0)
        log_norm = row_max + jnp.log(denominator)
        token_loss = log_norm - target_logit
        probabilities = jnp.exp(masked - log_norm[:, None])
        logit_grad = (
            token_grad[:, None] * (probabilities - onehot.astype(jnp.float32))
        ).astype(jnp.bfloat16)
        all_grads = lax.all_gather(logit_grad, "tok", axis=0, tiled=True)
        partial_value = lax.dot_general(
            all_grads,
            head_weight,
            (((1,), (1,)), ((), ())),
            preferred_element_type=jnp.float32,
        )
        blocks = (
            partial_value.reshape(tok_size, rows, share, feats)
            .transpose(0, 2, 1, 3)
            .reshape(vocab_size, rows, feats)
        )
        summed = lax.psum_scatter(blocks, "vocab", scatter_dimension=0, tiled=False)
        hidden_grad = lax.ppermute(summed.astype(jnp.bfloat16), ("vocab", "tok"), back)
        return (hidden_grad, token_loss)

    return on_device


GROUPS = 3
EXTRA = 128
BF = jnp.bfloat16
F32 = jnp.float32
I16 = jnp.int16


def schedule(groups):
    period, base = 29.5 / groups, 11.0
    took = {1: 0.0, 2: 3.0, 3: 3.0, 4: 3.0 + 8.4 / groups, 5: 4.7, 6: 2.2 + 8.4 / groups, 7: 1.3, 8: 4.5, 9: 4.5, 10: 4.5}
    events = []
    for g in range(groups):
        at = base + period * (g + 1)
        for step in range(1, 11):
            at += took[step]
            events.append((at, step, g))
    return [(step, g) for _, step, g in sorted(events)]


def kernel(
    groups,
    hidden_ref, weight_ref, targets_ref, mask_ref, grad_ref,
    out_ref, loss_ref,
    hid, wbuf, hb, plog, pin, xo, xi, msk, stats_out, stats_in, loss_rows, dl,
    mix_out, mix_in, near, eo, tin, fin,
    l_sem, w_sem, a_send, a_recv, x_send, x_recv, p_send, p_recv, c_send, c_recv,
    s_send, s_recv, d_send, d_recv, m_send, m_recv, e_send, f_recv, t_recv, r_send,
):
    rows, feats = hidden_ref.shape
    m = rows // groups
    width = weight_ref.shape[1]
    me_v = lax.axis_index("vocab")
    me_t = lax.axis_index("tok")
    z, x = me_v // 2, me_v % 2
    y, c = me_t // 2, me_t % 2
    nv = 8

    def dev(v, t):
        return {"vocab": v, "tok": t}

    def tok_of(r):
        return ((y + r // 2) % 2) * 2 + (c + r % 2) % 2

    other_x = z * 2 + (1 - x)

    def rcopy(src, dst, ss, rs, v, t):
        return pltpu.make_async_remote_copy(
            src_ref=src, dst_ref=dst, send_sem=ss, recv_sem=rs,
            device_id=dev(v, t), device_id_type=pl.DeviceIdType.MESH,
        )

    loads = [pltpu.make_async_copy(hidden_ref.at[pl.ds(g * m, m)], hid.at[g], l_sem.at[g]) for g in range(groups)]
    for load in loads:
        load.start()
    weights = pltpu.make_async_copy(weight_ref, wbuf, w_sem)
    weights.start()

    barrier = pltpu.get_barrier_semaphore()
    for k in range(4):
        for r in range(4):
            if k or r:
                pl.semaphore_signal(
                    barrier, inc=1, device_id=dev(((z + k) % 4) * 2 + x, tok_of(r)), device_id_type=pl.DeviceIdType.MESH
                )
        pl.semaphore_signal(
            barrier, inc=1, device_id=dev(((z + k) % 4) * 2 + 1 - x, me_t), device_id_type=pl.DeviceIdType.MESH
        )
    pl.semaphore_wait(barrier, 19)

    home = me_t == z

    def a_copy(g, zz):
        return rcopy(hid.at[g], hb.at[0, g, me_t], a_send.at[g, zz], a_recv.at[g, me_t], zz * 2 + x, z)

    def x_copy(g, t):
        return rcopy(hb.at[0, g, t], hb.at[1, g, t], x_send.at[g, t], x_recv.at[g, t], other_x, me_t)

    def x_own(g):
        return rcopy(hid.at[g], hb.at[1, g, me_t], x_send.at[g, me_t], x_recv.at[g, me_t], other_x, me_t)

    for g in range(groups):
        loads[g].wait()
        for k in (3, 2, 1):
            @pl.when(z + k < 4)
            def _():
                a_copy(g, z + k).start()

            @pl.when(z - k >= 0)
            def _():
                a_copy(g, z - k).start()

        @pl.when(jnp.logical_not(home))
        def _():
            a_copy(g, z).start()

        @pl.when(home)
        def _():
            x_own(g).start()

    @pl.when(home)
    def _():
        for g in range(groups):
            hb[0, g, me_t] = hid[g]

    top = jnp.concatenate([targets_ref[...].astype(F32), grad_ref[...]], axis=0)
    top = jnp.concatenate([top, jnp.zeros((2, 256 - rows), F32)], axis=1)
    sides = jnp.transpose(jnp.concatenate([top, jnp.zeros((126, 256), F32)], axis=0))
    columns = me_v * width + lax.broadcasted_iota(jnp.int32, (m, width), 1)

    def onehot_of(g):
        return columns == sides[g * m:(g + 1) * m, 0:1].astype(jnp.int32)

    def weight_rows(q):
        owner = (x + q) % 2
        return pl.ds(pl.multiple_of(owner * feats, 128), feats)

    def pair_copy(g, k):
        return rcopy(plog.at[g, tok_of(1 + 2 * k)], pin.at[g, k], p_send.at[g, k], p_recv.at[g, k], me_v, tok_of(1))

    def cross_copy(g):
        return rcopy(xo.at[g], xi.at[g], c_send.at[g], c_recv.at[g], me_v, tok_of(2))

    def stat_copy(g, k):
        return rcopy(stats_out.at[g], stats_in.at[g, me_v], s_send.at[g, k], s_recv.at[g, me_v], (me_v + k) % nv, me_t)

    def grad_copy(g, i):
        t = tok_of(2) if i == 2 else me_t
        return rcopy(dl.at[g, t], dl.at[g, t], d_send.at[g, i], d_recv.at[g, i], me_v, tok_of(2 if i == 0 else 1))

    def mix_copy(g, t):
        return rcopy(mix_out.at[g, t], mix_in.at[g, t], m_send.at[g, t], m_recv.at[g, t], other_x, me_t)

    def pass_copy(g, t):
        return rcopy(eo.at[g, t], tin.at[g, c], e_send.at[g, t], t_recv.at[g, c], me_v, t)

    def near_copy(g, t):
        return rcopy(eo.at[g, t], fin.at[g, z], e_send.at[g, t], f_recv.at[g, z], me_v, t)

    def far_copy(g, t):
        return rcopy(eo.at[g, t], fin.at[g, z], e_send.at[g, t], f_recv.at[g, z], me_t * 2 + x, t)

    def relay_copy(g, cc):
        return rcopy(tin.at[g, cc], fin.at[g, z], r_send.at[g, cc], f_recv.at[g, z], ((1 - y) * 2 + cc) * 2 + x, me_t)

    tile = 256

    def spread(g):
        for t in range(4):
            @pl.when(jnp.logical_not(home & (me_t == t)))
            def _():
                a_copy_in = rcopy(hid.at[g], hb.at[0, g, t], a_send.at[g, 0], a_recv.at[g, t], me_v, t)
                a_copy_in.wait_recv()
                x_copy(g, t).start()

    def logits_of(g):
        if g == 0:
            weights.wait()
        for t in range(4):
            x_copy(g, t).wait_recv()

        @pl.loop(0, width // tile)
        def _(j):
            cols = pl.ds(pl.multiple_of(j * tile, tile), tile)
            total = None
            for q in range(2):
                lhs = hb[q, g].reshape(4 * m, feats)
                term = jnp.dot(lhs, wbuf[weight_rows(q), cols], preferred_element_type=F32)
                total = term if total is None else total + term
            plog[g, :, :, cols] = total.reshape(4, m, tile)

        pair_copy(g, 1).start()
        pair_copy(g, 0).start()

    def cross_over(g):
        pair_copy(g, 1).wait_recv()
        value = plog[g, tok_of(2)] + pin[g, 1]
        top_of = jnp.max(jnp.abs(value), axis=1, keepdims=True)
        power = jnp.ceil(jnp.log2(jnp.maximum(top_of, jnp.float32(1e-20))) + jnp.float32(0.001))
        coded = jnp.round(value * jnp.exp2(15.0 - power)).astype(jnp.int32)
        xo[g, :, 0:width] = coded.astype(I16)
        xo[g, :, width:width + EXTRA] = jnp.broadcast_to(power.astype(jnp.int32), (m, EXTRA)).astype(I16)
        cross_copy(g).start()

    def softmax_of(g):
        pair_copy(g, 0).wait_recv()
        near_half = plog[g, me_t] + pin[g, 0]
        cross_copy(g).wait_recv()
        power = xi[g, :, width:width + EXTRA].astype(jnp.int32).astype(F32)[:, 0:1]
        logits = near_half + xi[g, :, 0:width].astype(jnp.int32).astype(F32) * jnp.exp2(power - 15.0)
        masked = jnp.where(mask_ref[...] == 1, logits, jnp.float32(-1e30))
        local_max = jnp.max(masked, axis=1, keepdims=True)
        local_target = jnp.sum(jnp.where(onehot_of(g), logits, 0.0), axis=1, keepdims=True)
        local_sum = jnp.sum(jnp.exp(masked - local_max), axis=1, keepdims=True)
        lanes = lax.broadcasted_iota(jnp.int32, (m, 128), 1)
        packed = jnp.where(lanes == 0, local_max, jnp.where(lanes == 1, local_sum, local_target))
        if m < 128:
            packed = jnp.concatenate([packed, jnp.zeros((128 - m, 128), F32)], axis=0)
        mine = jnp.transpose(packed)[0:8]
        stats_out[g] = mine
        stats_in[g, me_v] = mine
        msk[g] = masked
        for k in range(1, nv):
            stat_copy(g, k).start()

    def grads_of(g):
        for k in range(1, nv):
            source = (me_v + nv - k) % nv
            rcopy(stats_out.at[g], stats_in.at[g, source], s_send.at[g, k], s_recv.at[g, source], source, me_t).wait_recv()
        row_max = stats_in[g, 0][0:1]
        for v in range(1, nv):
            row_max = jnp.maximum(row_max, stats_in[g, v][0:1])
        denominator = jnp.zeros_like(row_max)
        target_logit = jnp.zeros_like(row_max)
        for v in range(nv):
            got = stats_in[g, v]
            denominator += got[1:2] * jnp.exp(got[0:1] - row_max)
            target_logit += got[2:3]
        log_norm = row_max + jnp.log(denominator)
        loss_rows[g] = log_norm - target_logit
        column = jnp.transpose(jnp.broadcast_to(log_norm, (128, 128)))[0:m, 0:1]
        probabilities = jnp.exp(msk[g] - column)
        tok_grad = sides[g * m:(g + 1) * m, 1:2]
        dl[g, me_t] = (tok_grad * (probabilities - onehot_of(g).astype(F32))).astype(BF)
        grad_copy(g, 0).start()
        grad_copy(g, 1).start()

    def grads_on(g):
        t = tok_of(2)
        rcopy(dl.at[g, t], dl.at[g, t], d_send.at[g, 0], d_recv.at[g, 0], me_v, t).wait_recv()
        grad_copy(g, 2).start()

    def terms_of(g):
        for i, r in ((1, 1), (2, 3)):
            t = tok_of(r)
            rcopy(dl.at[g, t], dl.at[g, t], d_send.at[g, i], d_recv.at[g, i], me_v, tok_of(1)).wait_recv()
        lhs = dl[g].reshape(4 * m, width)
        for q in (1, 0):
            value = lax.dot_general(
                lhs, wbuf[weight_rows(q), :], (((1,), (1,)), ((), ())), preferred_element_type=F32
            ).reshape(4, m, feats)
            if q == 0:
                near[g] = value
            else:
                mix_out[g] = value.astype(BF)
                for r in (2, 3, 1, 0):
                    mix_copy(g, tok_of(r)).start()

    def mixed(g):
        for r in (2, 3, 1, 0):
            t = tok_of(r)
            mix_copy(g, t).wait_recv()
            both = (near[g, t] + mix_in[g, t].astype(F32)).astype(BF)
            if r == 0:
                @pl.when(home)
                def _():
                    fin[g, z] = both

                @pl.when(jnp.logical_not(home))
                def _():
                    eo[g, t] = both
                    far_copy(g, t).start()
            elif r == 1:
                eo[g, t] = both
                far_copy(g, t).start()
            else:
                eo[g, t] = both

                @pl.when(home)
                def _():
                    near_copy(g, t).start()

                @pl.when(jnp.logical_not(home))
                def _():
                    pass_copy(g, t).start()

    def relayed(g):
        for cc in range(2):
            @pl.when((1 - y) * 2 + cc != z)
            def _():
                rcopy(eo.at[g, 0], tin.at[g, cc], e_send.at[g, 0], t_recv.at[g, cc], me_v, (1 - y) * 2 + cc).wait_recv()
                relay_copy(g, cc).start()

    def finish(g):
        total = None
        for zz in range(4):
            @pl.when(jnp.logical_not(home & (z == zz)))
            def _():
                rcopy(eo.at[g, 0], fin.at[g, zz], e_send.at[g, 0], f_recv.at[g, zz], zz * 2 + x, me_t).wait_recv()
        for zz in range(4):
            term = fin[g, zz].astype(F32)
            total = term if total is None else total + term
        out_ref[pl.ds(g * m, m), :] = total.astype(BF)

    steps = (spread, logits_of, cross_over, softmax_of, grads_of, grads_on, terms_of, mixed, relayed, finish)
    for step, g in schedule(groups):
        steps[step - 1](g)

    loss_ref[...] = jnp.concatenate([loss_rows[g][:, 0:m] for g in range(groups)], axis=1)

    for g in range(groups):
        for k in (3, 2, 1):
            @pl.when(z + k < 4)
            def _():
                a_copy(g, z + k).wait_send()

            @pl.when(z - k >= 0)
            def _():
                a_copy(g, z - k).wait_send()

        @pl.when(jnp.logical_not(home))
        def _():
            a_copy(g, z).wait_send()

        for t in range(4):
            x_copy(g, t).wait_send()
            mix_copy(g, t).wait_send()

            @pl.when(jnp.logical_not(home & (me_t == t)))
            def _():
                pass_copy(g, t).wait_send()

        for k in range(2):
            pair_copy(g, k).wait_send()

            @pl.when((1 - y) * 2 + k != z)
            def _():
                relay_copy(g, k).wait_send()

        cross_copy(g).wait_send()
        for k in range(1, nv):
            stat_copy(g, k).wait_send()
        for i in range(3):
            grad_copy(g, i).wait_send()


def fused(vocab_size, tok_size):
    def on_device(hidden, head_weight, targets, vocab_mask, token_grad):
        rows, feats = hidden.shape
        width = head_weight.shape[1]
        groups = GROUPS
        m = rows // groups
        dma = pltpu.SemaphoreType.DMA
        vmem = pl.BlockSpec(memory_space=pltpu.VMEM)
        hbm = pl.BlockSpec(memory_space=pltpu.HBM)
        hidden_grad, loss = pl.pallas_call(
            lambda *refs: kernel(groups, *refs),
            out_shape=(
                jax.ShapeDtypeStruct((rows, feats), BF),
                jax.ShapeDtypeStruct((1, rows), F32),
            ),
            in_specs=[hbm, hbm] + [vmem] * 3,
            out_specs=(vmem, vmem),
            scratch_shapes=[
                pltpu.VMEM((groups, m, feats), BF),
                pltpu.VMEM((2 * feats, width), BF),
                pltpu.VMEM((2, groups, 4, m, feats), BF),
                pltpu.VMEM((groups, 4, m, width), F32),
                pltpu.VMEM((groups, 2, m, width), F32),
                pltpu.VMEM((groups, m, width + EXTRA), I16),
                pltpu.VMEM((groups, m, width + EXTRA), I16),
                pltpu.VMEM((groups, m, width), F32),
                pltpu.VMEM((groups, 8, 128), F32),
                pltpu.VMEM((groups, vocab_size, 8, 128), F32),
                pltpu.VMEM((groups, 1, 128), F32),
                pltpu.VMEM((groups, 4, m, width), BF),
                pltpu.VMEM((groups, 4, m, feats), BF),
                pltpu.VMEM((groups, 4, m, feats), BF),
                pltpu.VMEM((groups, 4, m, feats), F32),
                pltpu.VMEM((groups, 4, m, feats), BF),
                pltpu.VMEM((groups, 2, m, feats), BF),
                pltpu.VMEM((groups, 4, m, feats), BF),
                dma((groups,)), dma,
                dma((groups, 4)), dma((groups, 4)), dma((groups, 4)), dma((groups, 4)),
                dma((groups, 2)), dma((groups, 2)), dma((groups,)), dma((groups,)),
                dma((groups, 8)), dma((groups, 8)), dma((groups, 3)), dma((groups, 3)),
                dma((groups, 4)), dma((groups, 4)), dma((groups, 4)), dma((groups, 4)),
                dma((groups, 2)), dma((groups, 2)),
            ],
            compiler_params=pltpu.CompilerParams(
                collective_id=0, has_side_effects=True, vmem_limit_bytes=60 * 1024 * 1024
            ),
        )(hidden, head_weight, targets[None, :], vocab_mask[None, :], token_grad[None, :])
        return (hidden_grad, loss.reshape(rows))

    return on_device


def solution(mesh):
    placed = (P("tok", "vocab"), P("tok", "vocab"), P("tok"), P("vocab"), P("tok"))
    vocab_size, tok_size = mesh.shape["vocab"], mesh.shape["tok"]

    def body(hidden, head_weight, *rest):
        rows, feats = hidden.shape
        fits = tok_size == 4 and vocab_size == 8 and feats % 128 == 0 and head_weight.shape[1] % 256 == 0
        fits = fits and rows <= 256 and rows % (16 * GROUPS) == 0 and rows <= 128 * GROUPS
        build = fused if fits else make_on_device
        return build(vocab_size, tok_size)(hidden, head_weight, *rest)

    return jax.shard_map(
        body,
        mesh=mesh,
        in_specs=placed,
        out_specs=(P("tok", "vocab"), P("tok")),
        check_vma=False,
    )
```

```python
import jax
import jax.numpy as jnp
from jax import lax
from jax.experimental import pallas as pl
from jax.experimental.pallas import tpu as pltpu
from jax.sharding import PartitionSpec as P


def make_on_device(vocab_size, tok_size):
    share = vocab_size // tok_size
    moves = [
        (b * tok_size + a, (a * share + b % share) * tok_size + b // share)
        for a in range(tok_size)
        for b in range(vocab_size)
    ]
    back = [(there, here) for here, there in moves]

    def on_device(hidden, head_weight, targets, vocab_mask, token_grad):
        rows, feats = hidden.shape
        block_width = head_weight.shape[1]
        moved = lax.ppermute(hidden, ("vocab", "tok"), moves)
        pieces = lax.all_gather(moved, "vocab")
        gathered = (
            pieces.reshape(tok_size, share, rows, feats)
            .transpose(0, 2, 1, 3)
            .reshape(tok_size * rows, share * feats)
        )
        partial_logits = jnp.dot(gathered, head_weight, preferred_element_type=jnp.float32)
        logits = lax.psum_scatter(partial_logits, "tok", scatter_dimension=0, tiled=True)
        first_column = lax.axis_index("vocab") * block_width
        masked = jnp.where(vocab_mask[None, :] == 1, logits, jnp.float32(-1e30))
        local_max = jnp.max(masked, axis=1)
        columns = first_column + jnp.arange(block_width, dtype=jnp.int32)
        onehot = columns[None, :] == targets[:, None]
        local_target = jnp.sum(jnp.where(onehot, logits, jnp.float32(0.0)), axis=1)
        weights = jnp.exp(masked - local_max[:, None])
        local_sum = jnp.sum(weights, axis=1)
        stats = lax.all_gather(jnp.stack([local_max, local_sum, local_target]), "vocab")
        row_max = jnp.max(stats[:, 0], axis=0)
        denominator = jnp.sum(stats[:, 1] * jnp.exp(stats[:, 0] - row_max[None]), axis=0)
        target_logit = jnp.sum(stats[:, 2], axis=0)
        log_norm = row_max + jnp.log(denominator)
        token_loss = log_norm - target_logit
        probabilities = jnp.exp(masked - log_norm[:, None])
        logit_grad = (
            token_grad[:, None] * (probabilities - onehot.astype(jnp.float32))
        ).astype(jnp.bfloat16)
        all_grads = lax.all_gather(logit_grad, "tok", axis=0, tiled=True)
        partial_value = lax.dot_general(
            all_grads,
            head_weight,
            (((1,), (1,)), ((), ())),
            preferred_element_type=jnp.float32,
        )
        blocks = (
            partial_value.reshape(tok_size, rows, share, feats)
            .transpose(0, 2, 1, 3)
            .reshape(vocab_size, rows, feats)
        )
        summed = lax.psum_scatter(blocks, "vocab", scatter_dimension=0, tiled=False)
        hidden_grad = lax.ppermute(summed.astype(jnp.bfloat16), ("vocab", "tok"), back)
        return (hidden_grad, token_loss)

    return on_device


SIZES = (64, 64, 64)
EXTRA = 128
BF = jnp.bfloat16
F32 = jnp.float32
I16 = jnp.int16


PLAN = """
ga0 ga1 sp0 ga2 sp1 lg0 co0 sp2 lg1 sm0 co1 gr0 lg2 sm1 go0 co2
tm0 gr1 sm2 go1 m20 m30 tm1 m10 m00 r00 r10 gr2 m21 m31 go2 tm2
m11 m01 r01 r11 fi0 m22 m32 m12 m02 r02 r12 fi1 fi2
"""


def kernel(
    sizes,
    hidden_ref, weight_ref, targets_ref, mask_ref, grad_ref,
    out_ref, loss_ref,
    hid, wbuf, hb, plog, pin, xo, xi, msk, stats_out, stats_in, loss_rows, dl,
    mix_out, mix_in, near, eo, tin, fin,
    l_sem, w_sem, a_send, a_recv, x_send, x_recv, p_send, p_recv, c_send, c_recv,
    s_send, s_recv, d_send, d_recv, m_send, m_recv, e_send, f_recv, t_recv, r_send,
):
    rows, feats = hidden_ref.shape
    groups = len(sizes)
    firsts = [sum(sizes[:g]) for g in range(groups)]
    width = weight_ref.shape[1]
    me_v = lax.axis_index("vocab")
    me_t = lax.axis_index("tok")
    z, x = me_v // 2, me_v % 2
    y, c = me_t // 2, me_t % 2
    nv = 8

    def dev(v, t):
        return {"vocab": v, "tok": t}

    def tok_of(r):
        return ((y + r // 2) % 2) * 2 + (c + r % 2) % 2

    other_x = z * 2 + (1 - x)

    def rcopy(src, dst, ss, rs, v, t):
        return pltpu.make_async_remote_copy(
            src_ref=src, dst_ref=dst, send_sem=ss, recv_sem=rs,
            device_id=dev(v, t), device_id_type=pl.DeviceIdType.MESH,
        )

    def span(g):
        return pl.ds(firsts[g], sizes[g])

    loads = [pltpu.make_async_copy(hidden_ref.at[span(g)], hid.at[span(g)], l_sem.at[g]) for g in range(groups)]
    for load in loads:
        load.start()
    weights = pltpu.make_async_copy(weight_ref, wbuf, w_sem)
    weights.start()

    barrier = pltpu.get_barrier_semaphore()
    for k in range(4):
        for r in range(4):
            if k or r:
                pl.semaphore_signal(
                    barrier, inc=1, device_id=dev(((z + k) % 4) * 2 + x, tok_of(r)), device_id_type=pl.DeviceIdType.MESH
                )
        pl.semaphore_signal(
            barrier, inc=1, device_id=dev(((z + k) % 4) * 2 + 1 - x, me_t), device_id_type=pl.DeviceIdType.MESH
        )
    pl.semaphore_wait(barrier, 19)

    home = me_t == z

    def a_copy(g, zz):
        return rcopy(hid.at[span(g)], hb.at[0, me_t, span(g)], a_send.at[g, zz], a_recv.at[g, me_t], zz * 2 + x, z)

    def x_copy(g, t):
        return rcopy(hb.at[0, t, span(g)], hb.at[1, t, span(g)], x_send.at[g, t], x_recv.at[g, t], other_x, me_t)

    def x_own(g):
        return rcopy(hid.at[span(g)], hb.at[1, me_t, span(g)], x_send.at[g, me_t], x_recv.at[g, me_t], other_x, me_t)

    def gather(g):
        loads[g].wait()
        for k in (1, 2, 3):
            @pl.when(z + k < 4)
            def _():
                a_copy(g, z + k).start()

            @pl.when(z - k >= 0)
            def _():
                a_copy(g, z - k).start()

        @pl.when(jnp.logical_not(home))
        def _():
            a_copy(g, z).start()

        @pl.when(home)
        def _():
            x_own(g).start()


    top = jnp.concatenate([targets_ref[...].astype(F32), grad_ref[...]], axis=0)
    top = jnp.concatenate([top, jnp.zeros((2, 256 - rows), F32)], axis=1)
    sides = jnp.transpose(jnp.concatenate([top, jnp.zeros((126, 256), F32)], axis=0))

    def onehot_of(g):
        columns = me_v * width + lax.broadcasted_iota(jnp.int32, (sizes[g], width), 1)
        return columns == sides[firsts[g]:firsts[g] + sizes[g], 0:1].astype(jnp.int32)

    def weight_rows(q):
        owner = (x + q) % 2
        return pl.ds(pl.multiple_of(owner * feats, 128), feats)

    def pair_copy(g, k):
        return rcopy(plog.at[tok_of(1 + 2 * k), span(g)], pin.at[k, span(g)], p_send.at[g, k], p_recv.at[g, k], me_v, tok_of(1))

    def cross_copy(g):
        return rcopy(xo.at[span(g)], xi.at[span(g)], c_send.at[g], c_recv.at[g], me_v, tok_of(2))

    def stat_copy(g, k):
        return rcopy(stats_out.at[g], stats_in.at[g, me_v], s_send.at[g, k], s_recv.at[g, me_v], (me_v + k) % nv, me_t)

    def grad_copy(g, i):
        t = tok_of(2) if i == 2 else me_t
        return rcopy(dl.at[t, span(g)], dl.at[t, span(g)], d_send.at[g, i], d_recv.at[g, i], me_v, tok_of(2 if i == 0 else 1))

    def mix_copy(g, t):
        return rcopy(mix_out.at[t, span(g)], mix_in.at[t, span(g)], m_send.at[g, t], m_recv.at[g, t], other_x, me_t)

    def pass_copy(g, t):
        return rcopy(eo.at[t, span(g)], tin.at[c, span(g)], e_send.at[g, t], t_recv.at[g, c], me_v, t)

    def near_copy(g, t):
        return rcopy(eo.at[t, span(g)], fin.at[z, span(g)], e_send.at[g, t], f_recv.at[g, z], me_v, t)

    def far_copy(g, t):
        return rcopy(eo.at[t, span(g)], fin.at[z, span(g)], e_send.at[g, t], f_recv.at[g, z], me_t * 2 + x, t)

    def relay_copy(g, cc):
        return rcopy(tin.at[cc, span(g)], fin.at[z, span(g)], r_send.at[g, cc], f_recv.at[g, z], ((1 - y) * 2 + cc) * 2 + x, me_t)

    tile = 256

    def spread(g):
        @pl.when(home)
        def _():
            hb[0, me_t, span(g)] = hid[span(g)]

        for t in range(4):
            @pl.when(jnp.logical_not(home & (me_t == t)))
            def _():
                a_copy_in = rcopy(hid.at[span(g)], hb.at[0, t, span(g)], a_send.at[g, 0], a_recv.at[g, t], me_v, t)
                a_copy_in.wait_recv()
                x_copy(g, t).start()

    def logits_of(g):
        if g == 0:
            weights.wait()
        for t in range(4):
            x_copy(g, t).wait_recv()

        @pl.loop(0, width // tile)
        def _(j):
            cols = pl.ds(pl.multiple_of(j * tile, tile), tile)
            total = None
            for q in range(2):
                lhs = hb[q, :, span(g), :].reshape(4 * sizes[g], feats)
                term = jnp.dot(lhs, wbuf[weight_rows(q), cols], preferred_element_type=F32)
                total = term if total is None else total + term
            plog[:, span(g), cols] = total.reshape(4, sizes[g], tile)

        pair_copy(g, 1).start()
        pair_copy(g, 0).start()

    def cross_over(g):
        pair_copy(g, 1).wait_recv()
        value = plog[tok_of(2), span(g), :] + pin[1, span(g), :]
        top_of = jnp.max(jnp.abs(value), axis=1, keepdims=True)
        power = jnp.ceil(jnp.log2(jnp.maximum(top_of, jnp.float32(1e-20))) + jnp.float32(0.001))
        coded = jnp.round(value * jnp.exp2(15.0 - power)).astype(jnp.int32)
        xo[span(g), 0:width] = coded.astype(I16)
        xo[span(g), width:width + EXTRA] = jnp.broadcast_to(power.astype(jnp.int32), (sizes[g], EXTRA)).astype(I16)
        cross_copy(g).start()

    def softmax_of(g):
        pair_copy(g, 0).wait_recv()
        near_half = plog[me_t, span(g), :] + pin[0, span(g), :]
        cross_copy(g).wait_recv()
        power = xi[span(g), width:width + EXTRA].astype(jnp.int32).astype(F32)[:, 0:1]
        logits = near_half + xi[span(g), 0:width].astype(jnp.int32).astype(F32) * jnp.exp2(power - 15.0)
        masked = jnp.where(mask_ref[...] == 1, logits, jnp.float32(-1e30))
        local_max = jnp.max(masked, axis=1, keepdims=True)
        local_target = jnp.sum(jnp.where(onehot_of(g), logits, 0.0), axis=1, keepdims=True)
        local_sum = jnp.sum(jnp.exp(masked - local_max), axis=1, keepdims=True)
        m = sizes[g]
        lanes = lax.broadcasted_iota(jnp.int32, (m, 128), 1)
        packed = jnp.where(lanes == 0, local_max, jnp.where(lanes == 1, local_sum, local_target))
        if m < 128:
            packed = jnp.concatenate([packed, jnp.zeros((128 - m, 128), F32)], axis=0)
        mine = jnp.transpose(packed)[0:8]
        stats_out[g] = mine
        stats_in[g, me_v] = mine
        msk[span(g), :] = masked
        for k in range(1, nv):
            stat_copy(g, k).start()

    def grads_of(g):
        for k in range(1, nv):
            source = (me_v + nv - k) % nv
            rcopy(stats_out.at[g], stats_in.at[g, source], s_send.at[g, k], s_recv.at[g, source], source, me_t).wait_recv()
        row_max = stats_in[g, 0][0:1]
        for v in range(1, nv):
            row_max = jnp.maximum(row_max, stats_in[g, v][0:1])
        denominator = jnp.zeros_like(row_max)
        target_logit = jnp.zeros_like(row_max)
        for v in range(nv):
            got = stats_in[g, v]
            denominator += got[1:2] * jnp.exp(got[0:1] - row_max)
            target_logit += got[2:3]
        log_norm = row_max + jnp.log(denominator)
        loss_rows[g] = log_norm - target_logit
        column = jnp.transpose(jnp.broadcast_to(log_norm, (128, 128)))[0:sizes[g], 0:1]
        probabilities = jnp.exp(msk[span(g), :] - column)
        tok_grad = sides[firsts[g]:firsts[g] + sizes[g], 1:2]
        dl[me_t, span(g), :] = (tok_grad * (probabilities - onehot_of(g).astype(F32))).astype(BF)
        grad_copy(g, 0).start()
        grad_copy(g, 1).start()

    def grads_on(g):
        t = tok_of(2)
        rcopy(dl.at[t, span(g)], dl.at[t, span(g)], d_send.at[g, 0], d_recv.at[g, 0], me_v, t).wait_recv()
        grad_copy(g, 2).start()

    def terms_of(g):
        for i, r in ((1, 1), (2, 3)):
            t = tok_of(r)
            rcopy(dl.at[t, span(g)], dl.at[t, span(g)], d_send.at[g, i], d_recv.at[g, i], me_v, tok_of(1)).wait_recv()
        lhs = dl[:, span(g), :].reshape(4 * sizes[g], width)
        for q in (1, 0):
            value = lax.dot_general(
                lhs, wbuf[weight_rows(q), :], (((1,), (1,)), ((), ())), preferred_element_type=F32
            ).reshape(4, sizes[g], feats)
            if q == 0:
                near[:, span(g), :] = value
            else:
                mix_out[:, span(g), :] = value.astype(BF)
                for r in (2, 3, 1, 0):
                    mix_copy(g, tok_of(r)).start()

    def mixed(g, r):
        t = tok_of(r)
        mix_copy(g, t).wait_recv()
        both = (near[t, span(g), :] + mix_in[t, span(g), :].astype(F32)).astype(BF)
        if r == 0:
            @pl.when(home)
            def _():
                fin[z, span(g), :] = both

            @pl.when(jnp.logical_not(home))
            def _():
                eo[t, span(g), :] = both
                far_copy(g, t).start()
        elif r == 1:
            eo[t, span(g), :] = both
            far_copy(g, t).start()
        else:
            eo[t, span(g), :] = both

            @pl.when(home)
            def _():
                near_copy(g, t).start()

            @pl.when(jnp.logical_not(home))
            def _():
                pass_copy(g, t).start()

    def relayed(g, r):
        cc = (c + r) % 2

        @pl.when((1 - y) * 2 + cc != z)
        def _():
            rcopy(eo.at[0, span(g)], tin.at[cc, span(g)], e_send.at[g, 0], t_recv.at[g, cc], me_v, (1 - y) * 2 + cc).wait_recv()
            relay_copy(g, cc).start()

    def finish(g):
        total = None
        for zz in range(4):
            @pl.when(jnp.logical_not(home & (z == zz)))
            def _():
                rcopy(eo.at[0, span(g)], fin.at[zz, span(g)], e_send.at[g, 0], f_recv.at[g, zz], zz * 2 + x, me_t).wait_recv()
        for zz in range(4):
            term = fin[zz, span(g), :].astype(F32)
            total = term if total is None else total + term
        out_ref[span(g), :] = total.astype(BF)

    steps = {
        "ga": gather, "sp": spread, "lg": logits_of, "co": cross_over, "sm": softmax_of, "gr": grads_of, "go": grads_on,
        "tm": terms_of, "fi": finish,
    }
    for r in range(4):
        steps[f"m{r}"] = lambda g, r=r: mixed(g, r)
    for r in range(2):
        steps[f"r{r}"] = lambda g, r=r: relayed(g, r)
    for item in PLAN.split():
        steps[item[:2]](int(item[2:]))

    loss_ref[...] = jnp.concatenate([loss_rows[g][:, 0:sizes[g]] for g in range(groups)], axis=1)

    for g in range(groups):
        for k in (3, 2, 1):
            @pl.when(z + k < 4)
            def _():
                a_copy(g, z + k).wait_send()

            @pl.when(z - k >= 0)
            def _():
                a_copy(g, z - k).wait_send()

        @pl.when(jnp.logical_not(home))
        def _():
            a_copy(g, z).wait_send()

        for t in range(4):
            x_copy(g, t).wait_send()
            mix_copy(g, t).wait_send()

            @pl.when(jnp.logical_not(home & (me_t == t)))
            def _():
                pass_copy(g, t).wait_send()

        for k in range(2):
            pair_copy(g, k).wait_send()

            @pl.when((1 - y) * 2 + k != z)
            def _():
                relay_copy(g, k).wait_send()

        cross_copy(g).wait_send()
        for k in range(1, nv):
            stat_copy(g, k).wait_send()
        for i in range(3):
            grad_copy(g, i).wait_send()


def fused(vocab_size, tok_size):
    def on_device(hidden, head_weight, targets, vocab_mask, token_grad):
        rows, feats = hidden.shape
        width = head_weight.shape[1]
        groups = len(SIZES)
        dma = pltpu.SemaphoreType.DMA
        vmem = pl.BlockSpec(memory_space=pltpu.VMEM)
        hbm = pl.BlockSpec(memory_space=pltpu.HBM)
        hidden_grad, loss = pl.pallas_call(
            lambda *refs: kernel(SIZES, *refs),
            out_shape=(
                jax.ShapeDtypeStruct((rows, feats), BF),
                jax.ShapeDtypeStruct((1, rows), F32),
            ),
            in_specs=[hbm, hbm] + [vmem] * 3,
            out_specs=(vmem, vmem),
            scratch_shapes=[
                pltpu.VMEM((rows, feats), BF),
                pltpu.VMEM((2 * feats, width), BF),
                pltpu.VMEM((2, 4, rows, feats), BF),
                pltpu.VMEM((4, rows, width), F32),
                pltpu.VMEM((2, rows, width), F32),
                pltpu.VMEM((rows, width + EXTRA), I16),
                pltpu.VMEM((rows, width + EXTRA), I16),
                pltpu.VMEM((rows, width), F32),
                pltpu.VMEM((groups, 8, 128), F32),
                pltpu.VMEM((groups, vocab_size, 8, 128), F32),
                pltpu.VMEM((groups, 1, 128), F32),
                pltpu.VMEM((4, rows, width), BF),
                pltpu.VMEM((4, rows, feats), BF),
                pltpu.VMEM((4, rows, feats), BF),
                pltpu.VMEM((4, rows, feats), F32),
                pltpu.VMEM((4, rows, feats), BF),
                pltpu.VMEM((2, rows, feats), BF),
                pltpu.VMEM((4, rows, feats), BF),
                dma((groups,)), dma,
                dma((groups, 4)), dma((groups, 4)), dma((groups, 4)), dma((groups, 4)),
                dma((groups, 2)), dma((groups, 2)), dma((groups,)), dma((groups,)),
                dma((groups, 8)), dma((groups, 8)), dma((groups, 3)), dma((groups, 3)),
                dma((groups, 4)), dma((groups, 4)), dma((groups, 4)), dma((groups, 4)),
                dma((groups, 2)), dma((groups, 2)),
            ],
            compiler_params=pltpu.CompilerParams(
                collective_id=0, has_side_effects=True, vmem_limit_bytes=60 * 1024 * 1024
            ),
        )(hidden, head_weight, targets[None, :], vocab_mask[None, :], token_grad[None, :])
        return (hidden_grad, loss.reshape(rows))

    return on_device


def solution(mesh):
    placed = (P("tok", "vocab"), P("tok", "vocab"), P("tok"), P("vocab"), P("tok"))
    vocab_size, tok_size = mesh.shape["vocab"], mesh.shape["tok"]

    def body(hidden, head_weight, *rest):
        rows, feats = hidden.shape
        fits = tok_size == 4 and vocab_size == 8 and feats % 128 == 0 and head_weight.shape[1] % 256 == 0
        fits = fits and rows <= 256 and rows == sum(SIZES)
        build = fused if fits else make_on_device
        return build(vocab_size, tok_size)(hidden, head_weight, *rest)

    return jax.shard_map(
        body,
        mesh=mesh,
        in_specs=placed,
        out_specs=(P("tok", "vocab"), P("tok")),
        check_vma=False,
    )
```

```python
import jax
import jax.numpy as jnp
from jax import lax
from jax.experimental import pallas as pl
from jax.experimental.pallas import tpu as pltpu
from jax.sharding import PartitionSpec as P


def make_on_device(vocab_size, tok_size):
    share = vocab_size // tok_size
    moves = [
        (b * tok_size + a, (a * share + b % share) * tok_size + b // share)
        for a in range(tok_size)
        for b in range(vocab_size)
    ]
    back = [(there, here) for here, there in moves]

    def on_device(hidden, head_weight, targets, vocab_mask, token_grad):
        rows, feats = hidden.shape
        block_width = head_weight.shape[1]
        moved = lax.ppermute(hidden, ("vocab", "tok"), moves)
        pieces = lax.all_gather(moved, "vocab")
        gathered = (
            pieces.reshape(tok_size, share, rows, feats)
            .transpose(0, 2, 1, 3)
            .reshape(tok_size * rows, share * feats)
        )
        partial_logits = jnp.dot(gathered, head_weight, preferred_element_type=jnp.float32)
        logits = lax.psum_scatter(partial_logits, "tok", scatter_dimension=0, tiled=True)
        first_column = lax.axis_index("vocab") * block_width
        masked = jnp.where(vocab_mask[None, :] == 1, logits, jnp.float32(-1e30))
        local_max = jnp.max(masked, axis=1)
        columns = first_column + jnp.arange(block_width, dtype=jnp.int32)
        onehot = columns[None, :] == targets[:, None]
        local_target = jnp.sum(jnp.where(onehot, logits, jnp.float32(0.0)), axis=1)
        weights = jnp.exp(masked - local_max[:, None])
        local_sum = jnp.sum(weights, axis=1)
        stats = lax.all_gather(jnp.stack([local_max, local_sum, local_target]), "vocab")
        row_max = jnp.max(stats[:, 0], axis=0)
        denominator = jnp.sum(stats[:, 1] * jnp.exp(stats[:, 0] - row_max[None]), axis=0)
        target_logit = jnp.sum(stats[:, 2], axis=0)
        log_norm = row_max + jnp.log(denominator)
        token_loss = log_norm - target_logit
        probabilities = jnp.exp(masked - log_norm[:, None])
        logit_grad = (
            token_grad[:, None] * (probabilities - onehot.astype(jnp.float32))
        ).astype(jnp.bfloat16)
        all_grads = lax.all_gather(logit_grad, "tok", axis=0, tiled=True)
        partial_value = lax.dot_general(
            all_grads,
            head_weight,
            (((1,), (1,)), ((), ())),
            preferred_element_type=jnp.float32,
        )
        blocks = (
            partial_value.reshape(tok_size, rows, share, feats)
            .transpose(0, 2, 1, 3)
            .reshape(vocab_size, rows, feats)
        )
        summed = lax.psum_scatter(blocks, "vocab", scatter_dimension=0, tiled=False)
        hidden_grad = lax.ppermute(summed.astype(jnp.bfloat16), ("vocab", "tok"), back)
        return (hidden_grad, token_loss)

    return on_device


SIZES = (32, 48, 48, 64)
EXTRA = 128
BF = jnp.bfloat16
F32 = jnp.float32
I16 = jnp.int16


PLAN = (
    "ga0", "ga1", "ld0", "ld1", "sp0", "ga2", "ga3", "ld2", "sp1", "sp2", "lg0", "ld3", "co0", "lg1", "sm0",
    "co1", "sp3", "lg2", "sm1", "co2", "gr0", "go0", "sm2", "tm0", "gr1", "lg3", "gr2", "m30", "m20", "go1",
    "tm1", "co3", "m10", "go2", "r00", "m00", "r10", "sm3", "m31", "m21", "m11", "r11", "tm2", "gr3", "r01",
    "m22", "m01", "go3", "tm3", "m32", "m12", "r02", "m23", "r12", "m02", "fi1", "m13", "m33", "r03", "r13",
    "fi2", "m03", "fi0", "fi3",
)


def kernel(
    sizes,
    hidden_ref, weight_ref, targets_ref, mask_ref, grad_ref,
    out_ref, loss_ref,
    hid, wbuf, land, hb, plog, pin, xo, xi, msk, stats_out, stats_in, loss_rows, dl,
    mix_out, mix_in, near, eo, tin, fin,
    l_sem, w_sem, a_send, a_recv, n_recv, n_send, x_send, x_recv, p_send, p_recv, c_send, c_recv,
    s_send, s_recv, d_send, d_recv, m_send, m_recv, e_send, f_recv, t_recv, r_send,
):
    rows, feats = hidden_ref.shape
    groups = len(sizes)
    firsts = [sum(sizes[:g]) for g in range(groups)]
    width = weight_ref.shape[1]
    me_v = lax.axis_index("vocab")
    me_t = lax.axis_index("tok")
    z, x = me_v // 2, me_v % 2
    y, c = me_t // 2, me_t % 2
    nv = 8

    def dev(v, t):
        return {"vocab": v, "tok": t}

    def tok_of(r):
        return ((y + r // 2) % 2) * 2 + (c + r % 2) % 2

    other_x = z * 2 + (1 - x)

    def rcopy(src, dst, ss, rs, v, t):
        return pltpu.make_async_remote_copy(
            src_ref=src, dst_ref=dst, send_sem=ss, recv_sem=rs,
            device_id=dev(v, t), device_id_type=pl.DeviceIdType.MESH,
        )

    def span(g):
        return pl.ds(firsts[g], sizes[g])

    loads = [pltpu.make_async_copy(hidden_ref.at[span(g)], hid.at[span(g)], l_sem.at[g]) for g in range(groups)]
    for load in loads:
        load.start()
    weights = pltpu.make_async_copy(weight_ref, wbuf, w_sem)
    weights.start()

    barrier = pltpu.get_barrier_semaphore()
    for k in range(4):
        for r in range(4):
            if k or r:
                pl.semaphore_signal(
                    barrier, inc=1, device_id=dev(((z + k) % 4) * 2 + x, tok_of(r)), device_id_type=pl.DeviceIdType.MESH
                )
        pl.semaphore_signal(
            barrier, inc=1, device_id=dev(((z + k) % 4) * 2 + 1 - x, me_t), device_id_type=pl.DeviceIdType.MESH
        )
    pl.semaphore_wait(barrier, 19)

    home = me_t == z

    side = z // 2
    partner = z + 1 - 2 * (z % 2)
    inner = jnp.where(z < 2, 2, 1)
    outer = jnp.where(z < 2, 0, 3)
    is_inner = (z == 1) | (z == 2)
    landed = is_inner & (me_t // 2 == 1 - side)

    def a_copy(g):
        return rcopy(hid.at[span(g)], hb.at[0, me_t, span(g)], a_send.at[g, 0], a_recv.at[g, me_t], partner * 2 + x, z)

    def n_copy(g):
        i = jnp.where(is_inner, 0, 1)
        return rcopy(hid.at[span(g)], land.at[i, span(g)], a_send.at[g, 1], n_recv.at[g, i], inner * 2 + x, me_t)

    def o_copy(g):
        return rcopy(hid.at[span(g)], hb.at[0, me_t, span(g)], a_send.at[g, 2], a_recv.at[g, me_t], me_v, z)

    def landing(i):
        return jnp.where(z == 2, 1 - i, 2 + i)

    def n_out(g, i):
        return rcopy(
            land.at[i, span(g)], hb.at[0, me_t, span(g)], n_send.at[g, i, 0], a_recv.at[g, me_t], outer * 2 + x, landing(i)
        )

    def n_near(g, i):
        return rcopy(land.at[i, span(g)], hb.at[0, me_t, span(g)], n_send.at[g, i, 1], a_recv.at[g, me_t], me_v, landing(i))

    def n_own(g, i):
        return rcopy(land.at[i, span(g)], hb.at[1, me_t, span(g)], x_send.at[g, me_t], x_recv.at[g, me_t], other_x, me_t)

    def x_copy(g, t):
        return rcopy(hb.at[0, t, span(g)], hb.at[1, t, span(g)], x_send.at[g, t], x_recv.at[g, t], other_x, me_t)

    def x_own(g):
        return rcopy(hid.at[span(g)], hb.at[1, me_t, span(g)], x_send.at[g, me_t], x_recv.at[g, me_t], other_x, me_t)

    def gather(g):
        loads[g].wait()
        a_copy(g).start()
        n_copy(g).start()

        @pl.when(jnp.logical_not(home))
        def _():
            o_copy(g).start()

        @pl.when(home)
        def _():
            x_own(g).start()


    top = jnp.concatenate([targets_ref[...].astype(F32), grad_ref[...]], axis=0)
    top = jnp.concatenate([top, jnp.zeros((2, 256 - rows), F32)], axis=1)
    sides = jnp.transpose(jnp.concatenate([top, jnp.zeros((126, 256), F32)], axis=0))

    def onehot_of(g):
        columns = me_v * width + lax.broadcasted_iota(jnp.int32, (sizes[g], width), 1)
        return columns == sides[firsts[g]:firsts[g] + sizes[g], 0:1].astype(jnp.int32)

    def weight_rows(q):
        owner = (x + q) % 2
        return pl.ds(pl.multiple_of(owner * feats, 128), feats)

    def pair_copy(g, k):
        return rcopy(plog.at[tok_of(1 + 2 * k), span(g)], pin.at[k, span(g)], p_send.at[g, k], p_recv.at[g, k], me_v, tok_of(1))

    def cross_copy(g):
        return rcopy(xo.at[span(g)], xi.at[span(g)], c_send.at[g], c_recv.at[g], me_v, tok_of(2))

    def stat_copy(g, k):
        return rcopy(stats_out.at[g], stats_in.at[g, me_v], s_send.at[g, k], s_recv.at[g, me_v], (me_v + k) % nv, me_t)

    def grad_copy(g, i):
        t = tok_of(2) if i == 2 else me_t
        return rcopy(dl.at[t, span(g)], dl.at[t, span(g)], d_send.at[g, i], d_recv.at[g, i], me_v, tok_of(2 if i == 0 else 1))

    def mix_copy(g, t):
        return rcopy(mix_out.at[t, span(g)], mix_in.at[t, span(g)], m_send.at[g, t], m_recv.at[g, t], other_x, me_t)

    def pass_copy(g, t):
        return rcopy(eo.at[t, span(g)], tin.at[c, span(g)], e_send.at[g, t], t_recv.at[g, c], me_v, t)

    def near_copy(g, t):
        return rcopy(eo.at[t, span(g)], fin.at[z, span(g)], e_send.at[g, t], f_recv.at[g, z], me_v, t)

    def far_copy(g, t):
        return rcopy(eo.at[t, span(g)], fin.at[z, span(g)], e_send.at[g, t], f_recv.at[g, z], me_t * 2 + x, t)

    def relay_copy(g, cc):
        return rcopy(tin.at[cc, span(g)], fin.at[z, span(g)], r_send.at[g, cc], f_recv.at[g, z], ((1 - y) * 2 + cc) * 2 + x, me_t)

    tile = 256

    def passed(g):
        @pl.when(is_inner)
        def _():
            for i in range(2):
                rcopy(
                    hid.at[span(g)], land.at[i, span(g)], a_send.at[g, 1], n_recv.at[g, i], landing(i) * 2 + x, me_t
                ).wait_recv()
                n_out(g, i).start()

                @pl.when(landing(i) != me_t)
                def _():
                    n_near(g, i).start()

                @pl.when(landing(i) == me_t)
                def _():
                    n_own(g, i).start()
                    hb[0, me_t, span(g)] = land[i, span(g)]

    def spread(g):
        @pl.when(home)
        def _():
            hb[0, me_t, span(g)] = hid[span(g)]

        for t in range(4):
            @pl.when(jnp.logical_not((home | landed) & (me_t == t)))
            def _():
                a_copy_in = rcopy(hid.at[span(g)], hb.at[0, t, span(g)], a_send.at[g, 0], a_recv.at[g, t], me_v, t)
                a_copy_in.wait_recv()
                x_copy(g, t).start()

    def logits_of(g):
        if g == 0:
            weights.wait()
        for t in range(4):
            x_copy(g, t).wait_recv()

        @pl.loop(0, width // tile)
        def _(j):
            cols = pl.ds(pl.multiple_of(j * tile, tile), tile)
            total = None
            for q in range(2):
                lhs = hb[q, :, span(g), :].reshape(4 * sizes[g], feats)
                term = jnp.dot(lhs, wbuf[weight_rows(q), cols], preferred_element_type=F32)
                total = term if total is None else total + term
            plog[:, span(g), cols] = total.reshape(4, sizes[g], tile)

        pair_copy(g, 1).start()
        pair_copy(g, 0).start()

    def cross_over(g):
        pair_copy(g, 1).wait_recv()
        value = plog[tok_of(2), span(g), :] + pin[1, span(g), :]
        top_of = jnp.max(jnp.abs(value), axis=1, keepdims=True)
        power = jnp.ceil(jnp.log2(jnp.maximum(top_of, jnp.float32(1e-20))) + jnp.float32(0.001))
        coded = jnp.round(value * jnp.exp2(15.0 - power)).astype(jnp.int32)
        xo[span(g), 0:width] = coded.astype(I16)
        xo[span(g), width:width + EXTRA] = jnp.broadcast_to(power.astype(jnp.int32), (sizes[g], EXTRA)).astype(I16)
        cross_copy(g).start()

    def softmax_of(g):
        pair_copy(g, 0).wait_recv()
        near_half = plog[me_t, span(g), :] + pin[0, span(g), :]
        cross_copy(g).wait_recv()
        power = xi[span(g), width:width + EXTRA].astype(jnp.int32).astype(F32)[:, 0:1]
        logits = near_half + xi[span(g), 0:width].astype(jnp.int32).astype(F32) * jnp.exp2(power - 15.0)
        masked = jnp.where(mask_ref[...] == 1, logits, jnp.float32(-1e30))
        local_max = jnp.max(masked, axis=1, keepdims=True)
        local_target = jnp.sum(jnp.where(onehot_of(g), logits, 0.0), axis=1, keepdims=True)
        local_sum = jnp.sum(jnp.exp(masked - local_max), axis=1, keepdims=True)
        m = sizes[g]
        lanes = lax.broadcasted_iota(jnp.int32, (m, 128), 1)
        packed = jnp.where(lanes == 0, local_max, jnp.where(lanes == 1, local_sum, local_target))
        if m < 128:
            packed = jnp.concatenate([packed, jnp.zeros((128 - m, 128), F32)], axis=0)
        mine = jnp.transpose(packed)[0:8]
        stats_out[g] = mine
        stats_in[g, me_v] = mine
        msk[span(g), :] = masked
        for k in range(1, nv):
            stat_copy(g, k).start()

    def grads_of(g):
        for k in range(1, nv):
            source = (me_v + nv - k) % nv
            rcopy(stats_out.at[g], stats_in.at[g, source], s_send.at[g, k], s_recv.at[g, source], source, me_t).wait_recv()
        row_max = stats_in[g, 0][0:1]
        for v in range(1, nv):
            row_max = jnp.maximum(row_max, stats_in[g, v][0:1])
        denominator = jnp.zeros_like(row_max)
        target_logit = jnp.zeros_like(row_max)
        for v in range(nv):
            got = stats_in[g, v]
            denominator += got[1:2] * jnp.exp(got[0:1] - row_max)
            target_logit += got[2:3]
        log_norm = row_max + jnp.log(denominator)
        loss_rows[g] = log_norm - target_logit
        column = jnp.transpose(jnp.broadcast_to(log_norm, (128, 128)))[0:sizes[g], 0:1]
        probabilities = jnp.exp(msk[span(g), :] - column)
        tok_grad = sides[firsts[g]:firsts[g] + sizes[g], 1:2]
        dl[me_t, span(g), :] = (tok_grad * (probabilities - onehot_of(g).astype(F32))).astype(BF)
        grad_copy(g, 0).start()
        grad_copy(g, 1).start()

    def grads_on(g):
        t = tok_of(2)
        rcopy(dl.at[t, span(g)], dl.at[t, span(g)], d_send.at[g, 0], d_recv.at[g, 0], me_v, t).wait_recv()
        grad_copy(g, 2).start()

    def terms_of(g):
        for i, r in ((1, 1), (2, 3)):
            t = tok_of(r)
            rcopy(dl.at[t, span(g)], dl.at[t, span(g)], d_send.at[g, i], d_recv.at[g, i], me_v, tok_of(1)).wait_recv()
        lhs = dl[:, span(g), :].reshape(4 * sizes[g], width)
        for q in (1, 0):
            value = lax.dot_general(
                lhs, wbuf[weight_rows(q), :], (((1,), (1,)), ((), ())), preferred_element_type=F32
            ).reshape(4, sizes[g], feats)
            if q == 0:
                near[:, span(g), :] = value
            else:
                mix_out[:, span(g), :] = value.astype(BF)
                for r in (2, 3, 1, 0):
                    mix_copy(g, tok_of(r)).start()

    def mixed(g, r):
        t = tok_of(r)
        mix_copy(g, t).wait_recv()
        both = (near[t, span(g), :] + mix_in[t, span(g), :].astype(F32)).astype(BF)
        if r == 0:
            @pl.when(home)
            def _():
                fin[z, span(g), :] = both

            @pl.when(jnp.logical_not(home))
            def _():
                eo[t, span(g), :] = both
                far_copy(g, t).start()
        elif r == 1:
            eo[t, span(g), :] = both
            far_copy(g, t).start()
        else:
            eo[t, span(g), :] = both

            @pl.when(home)
            def _():
                near_copy(g, t).start()

            @pl.when(jnp.logical_not(home))
            def _():
                pass_copy(g, t).start()

    def relayed(g, r):
        cc = (c + r) % 2

        @pl.when((1 - y) * 2 + cc != z)
        def _():
            rcopy(eo.at[0, span(g)], tin.at[cc, span(g)], e_send.at[g, 0], t_recv.at[g, cc], me_v, (1 - y) * 2 + cc).wait_recv()
            relay_copy(g, cc).start()

    def finish(g):
        total = None
        for zz in range(4):
            @pl.when(jnp.logical_not(home & (z == zz)))
            def _():
                rcopy(eo.at[0, span(g)], fin.at[zz, span(g)], e_send.at[g, 0], f_recv.at[g, zz], zz * 2 + x, me_t).wait_recv()
        for zz in range(4):
            term = fin[zz, span(g), :].astype(F32)
            total = term if total is None else total + term
        out_ref[span(g), :] = total.astype(BF)

    steps = {
        "ga": gather, "ld": passed, "sp": spread, "lg": logits_of, "co": cross_over, "sm": softmax_of, "gr": grads_of, "go": grads_on,
        "tm": terms_of, "fi": finish,
    }
    for r in range(4):
        steps[f"m{r}"] = lambda g, r=r: mixed(g, r)
    for r in range(2):
        steps[f"r{r}"] = lambda g, r=r: relayed(g, r)
    for item in PLAN:
        steps[item[:2]](int(item[2:]))

    loss_ref[...] = jnp.concatenate([loss_rows[g][:, 0:sizes[g]] for g in range(groups)], axis=1)

    for g in range(groups):
        a_copy(g).wait_send()
        n_copy(g).wait_send()

        @pl.when(jnp.logical_not(home))
        def _():
            o_copy(g).wait_send()

        @pl.when(is_inner)
        def _():
            for i in range(2):
                n_out(g, i).wait_send()

                @pl.when(landing(i) != me_t)
                def _():
                    n_near(g, i).wait_send()

        for t in range(4):
            x_copy(g, t).wait_send()
            mix_copy(g, t).wait_send()

            @pl.when(jnp.logical_not(home & (me_t == t)))
            def _():
                pass_copy(g, t).wait_send()

        for k in range(2):
            pair_copy(g, k).wait_send()

            @pl.when((1 - y) * 2 + k != z)
            def _():
                relay_copy(g, k).wait_send()

        cross_copy(g).wait_send()
        for k in range(1, nv):
            stat_copy(g, k).wait_send()
        for i in range(3):
            grad_copy(g, i).wait_send()


def fused(vocab_size, tok_size):
    def on_device(hidden, head_weight, targets, vocab_mask, token_grad):
        rows, feats = hidden.shape
        width = head_weight.shape[1]
        groups = len(SIZES)
        dma = pltpu.SemaphoreType.DMA
        vmem = pl.BlockSpec(memory_space=pltpu.VMEM)
        hbm = pl.BlockSpec(memory_space=pltpu.HBM)
        hidden_grad, loss = pl.pallas_call(
            lambda *refs: kernel(SIZES, *refs),
            out_shape=(
                jax.ShapeDtypeStruct((rows, feats), BF),
                jax.ShapeDtypeStruct((1, rows), F32),
            ),
            in_specs=[hbm, hbm] + [vmem] * 3,
            out_specs=(vmem, vmem),
            scratch_shapes=[
                pltpu.VMEM((rows, feats), BF),
                pltpu.VMEM((2 * feats, width), BF),
                pltpu.VMEM((2, rows, feats), BF),
                pltpu.VMEM((2, 4, rows, feats), BF),
                pltpu.VMEM((4, rows, width), F32),
                pltpu.VMEM((2, rows, width), F32),
                pltpu.VMEM((rows, width + EXTRA), I16),
                pltpu.VMEM((rows, width + EXTRA), I16),
                pltpu.VMEM((rows, width), F32),
                pltpu.VMEM((groups, 8, 128), F32),
                pltpu.VMEM((groups, vocab_size, 8, 128), F32),
                pltpu.VMEM((groups, 1, 128), F32),
                pltpu.VMEM((4, rows, width), BF),
                pltpu.VMEM((4, rows, feats), BF),
                pltpu.VMEM((4, rows, feats), BF),
                pltpu.VMEM((4, rows, feats), F32),
                pltpu.VMEM((4, rows, feats), BF),
                pltpu.VMEM((2, rows, feats), BF),
                pltpu.VMEM((4, rows, feats), BF),
                dma((groups,)), dma,
                dma((groups, 3)), dma((groups, 4)), dma((groups, 2)), dma((groups, 2, 2)), dma((groups, 4)), dma((groups, 4)),
                dma((groups, 2)), dma((groups, 2)), dma((groups,)), dma((groups,)),
                dma((groups, 8)), dma((groups, 8)), dma((groups, 3)), dma((groups, 3)),
                dma((groups, 4)), dma((groups, 4)), dma((groups, 4)), dma((groups, 4)),
                dma((groups, 2)), dma((groups, 2)),
            ],
            compiler_params=pltpu.CompilerParams(
                collective_id=0, has_side_effects=True, vmem_limit_bytes=60 * 1024 * 1024
            ),
        )(hidden, head_weight, targets[None, :], vocab_mask[None, :], token_grad[None, :])
        return (hidden_grad, loss.reshape(rows))

    return on_device


def solution(mesh):
    placed = (P("tok", "vocab"), P("tok", "vocab"), P("tok"), P("vocab"), P("tok"))
    vocab_size, tok_size = mesh.shape["vocab"], mesh.shape["tok"]

    def body(hidden, head_weight, *rest):
        rows, feats = hidden.shape
        fits = tok_size == 4 and vocab_size == 8 and feats % 128 == 0 and head_weight.shape[1] % 256 == 0
        fits = fits and rows <= 256 and rows == sum(SIZES)
        build = fused if fits else make_on_device
        return build(vocab_size, tok_size)(hidden, head_weight, *rest)

    return jax.shard_map(
        body,
        mesh=mesh,
        in_specs=placed,
        out_specs=(P("tok", "vocab"), P("tok")),
        check_vma=False,
    )
```

```python
import jax
import jax.numpy as jnp
from jax import lax
from jax.experimental import pallas as pl
from jax.experimental.pallas import tpu as pltpu
from jax.sharding import PartitionSpec as P


def make_on_device(vocab_size, tok_size):
    share = vocab_size // tok_size
    moves = [
        (b * tok_size + a, (a * share + b % share) * tok_size + b // share)
        for a in range(tok_size)
        for b in range(vocab_size)
    ]
    back = [(there, here) for here, there in moves]

    def on_device(hidden, head_weight, targets, vocab_mask, token_grad):
        rows, feats = hidden.shape
        block_width = head_weight.shape[1]
        moved = lax.ppermute(hidden, ("vocab", "tok"), moves)
        pieces = lax.all_gather(moved, "vocab")
        gathered = (
            pieces.reshape(tok_size, share, rows, feats)
            .transpose(0, 2, 1, 3)
            .reshape(tok_size * rows, share * feats)
        )
        partial_logits = jnp.dot(gathered, head_weight, preferred_element_type=jnp.float32)
        logits = lax.psum_scatter(partial_logits, "tok", scatter_dimension=0, tiled=True)
        first_column = lax.axis_index("vocab") * block_width
        masked = jnp.where(vocab_mask[None, :] == 1, logits, jnp.float32(-1e30))
        local_max = jnp.max(masked, axis=1)
        columns = first_column + jnp.arange(block_width, dtype=jnp.int32)
        onehot = columns[None, :] == targets[:, None]
        local_target = jnp.sum(jnp.where(onehot, logits, jnp.float32(0.0)), axis=1)
        weights = jnp.exp(masked - local_max[:, None])
        local_sum = jnp.sum(weights, axis=1)
        stats = lax.all_gather(jnp.stack([local_max, local_sum, local_target]), "vocab")
        row_max = jnp.max(stats[:, 0], axis=0)
        denominator = jnp.sum(stats[:, 1] * jnp.exp(stats[:, 0] - row_max[None]), axis=0)
        target_logit = jnp.sum(stats[:, 2], axis=0)
        log_norm = row_max + jnp.log(denominator)
        token_loss = log_norm - target_logit
        probabilities = jnp.exp(masked - log_norm[:, None])
        logit_grad = (
            token_grad[:, None] * (probabilities - onehot.astype(jnp.float32))
        ).astype(jnp.bfloat16)
        all_grads = lax.all_gather(logit_grad, "tok", axis=0, tiled=True)
        partial_value = lax.dot_general(
            all_grads,
            head_weight,
            (((1,), (1,)), ((), ())),
            preferred_element_type=jnp.float32,
        )
        blocks = (
            partial_value.reshape(tok_size, rows, share, feats)
            .transpose(0, 2, 1, 3)
            .reshape(vocab_size, rows, feats)
        )
        summed = lax.psum_scatter(blocks, "vocab", scatter_dimension=0, tiled=False)
        hidden_grad = lax.ppermute(summed.astype(jnp.bfloat16), ("vocab", "tok"), back)
        return (hidden_grad, token_loss)

    return on_device


SIZES = (48, 48, 48, 48)
EXTRA = 128
BF = jnp.bfloat16
F32 = jnp.float32
I16 = jnp.int16


PLAN = (
    "ga0", "ld0", "ga1", "sp0", "ld1", "ga2", "sp1", "lg0", "ld2", "ga3", "sp2", "co0", "sm0", "lg1", "ld3",
    "co1", "sp3", "gr0", "sm1", "lg2", "go0", "co2", "tm0", "gr1", "lg3", "co3", "sm2", "m20", "go1", "tm1",
    "sm3", "m30", "r00", "m10", "gr2", "m00", "go2", "m31", "r10", "tm2", "m21", "m11", "gr3", "m01", "r11",
    "go3", "r01", "m32", "m12", "m22", "tm3", "m02", "r12", "r02", "m33", "m13", "m23", "fi0", "fi1", "m03",
    "r03", "r13", "fi2", "fi3",
)


def kernel(
    sizes,
    hidden_ref, weight_ref, targets_ref, mask_ref, grad_ref,
    out_ref, loss_ref,
    hid, wbuf, land, hb, plog, pin, xo, xi, msk, stats_out, stats_in, loss_rows, dl,
    mix_out, mix_in, near, eo, tin, fin,
    l_sem, w_sem, a_send, a_recv, n_recv, n_send, x_send, x_recv, p_send, p_recv, c_send, c_recv,
    s_send, s_recv, d_send, d_recv, m_send, m_recv, e_send, f_recv, t_recv, r_send,
):
    rows, feats = hidden_ref.shape
    groups = len(sizes)
    firsts = [sum(sizes[:g]) for g in range(groups)]
    width = weight_ref.shape[1]
    me_v = lax.axis_index("vocab")
    me_t = lax.axis_index("tok")
    z, x = me_v // 2, me_v % 2
    y, c = me_t // 2, me_t % 2
    nv = 8

    def dev(v, t):
        return {"vocab": v, "tok": t}

    def tok_of(r):
        return ((y + r // 2) % 2) * 2 + (c + r % 2) % 2

    other_x = z * 2 + (1 - x)

    def rcopy(src, dst, ss, rs, v, t):
        return pltpu.make_async_remote_copy(
            src_ref=src, dst_ref=dst, send_sem=ss, recv_sem=rs,
            device_id=dev(v, t), device_id_type=pl.DeviceIdType.MESH,
        )

    def span(g):
        return pl.ds(firsts[g], sizes[g])

    loads = [pltpu.make_async_copy(hidden_ref.at[span(g)], hid.at[span(g)], l_sem.at[g]) for g in range(groups)]
    for load in loads:
        load.start()
    weights = pltpu.make_async_copy(weight_ref, wbuf, w_sem)
    weights.start()

    barrier = pltpu.get_barrier_semaphore()
    for k in range(4):
        for r in range(4):
            if k or r:
                pl.semaphore_signal(
                    barrier, inc=1, device_id=dev(((z + k) % 4) * 2 + x, tok_of(r)), device_id_type=pl.DeviceIdType.MESH
                )
        pl.semaphore_signal(
            barrier, inc=1, device_id=dev(((z + k) % 4) * 2 + 1 - x, me_t), device_id_type=pl.DeviceIdType.MESH
        )
    pl.semaphore_wait(barrier, 19)

    home = me_t == z

    side = z // 2
    partner = z + 1 - 2 * (z % 2)
    inner = jnp.where(z < 2, 2, 1)
    outer = jnp.where(z < 2, 0, 3)
    is_inner = (z == 1) | (z == 2)
    landed = is_inner & (me_t // 2 == 1 - side)

    def a_copy(g):
        return rcopy(hid.at[span(g)], hb.at[0, me_t, span(g)], a_send.at[g, 0], a_recv.at[g, me_t], partner * 2 + x, z)

    def n_copy(g):
        i = jnp.where(is_inner, 0, 1)
        return rcopy(hid.at[span(g)], land.at[i, span(g)], a_send.at[g, 1], n_recv.at[g, i], inner * 2 + x, me_t)

    def o_copy(g):
        return rcopy(hid.at[span(g)], hb.at[0, me_t, span(g)], a_send.at[g, 2], a_recv.at[g, me_t], me_v, z)

    def landing(i):
        return jnp.where(z == 2, 1 - i, 2 + i)

    def n_out(g, i):
        return rcopy(
            land.at[i, span(g)], hb.at[0, me_t, span(g)], n_send.at[g, i, 0], a_recv.at[g, me_t], outer * 2 + x, landing(i)
        )

    def n_near(g, i):
        return rcopy(land.at[i, span(g)], hb.at[0, me_t, span(g)], n_send.at[g, i, 1], a_recv.at[g, me_t], me_v, landing(i))

    def n_own(g, i):
        return rcopy(land.at[i, span(g)], hb.at[1, me_t, span(g)], x_send.at[g, me_t], x_recv.at[g, me_t], other_x, me_t)

    def x_copy(g, t):
        return rcopy(hb.at[0, t, span(g)], hb.at[1, t, span(g)], x_send.at[g, t], x_recv.at[g, t], other_x, me_t)

    def x_own(g):
        return rcopy(hid.at[span(g)], hb.at[1, me_t, span(g)], x_send.at[g, me_t], x_recv.at[g, me_t], other_x, me_t)

    def gather(g):
        loads[g].wait()
        a_copy(g).start()
        n_copy(g).start()

        @pl.when(jnp.logical_not(home))
        def _():
            o_copy(g).start()

        @pl.when(home)
        def _():
            x_own(g).start()


    top = jnp.concatenate([targets_ref[...].astype(F32), grad_ref[...]], axis=0)
    top = jnp.concatenate([top, jnp.zeros((2, 256 - rows), F32)], axis=1)
    sides = jnp.transpose(jnp.concatenate([top, jnp.zeros((126, 256), F32)], axis=0))

    def onehot_of(g):
        columns = me_v * width + lax.broadcasted_iota(jnp.int32, (sizes[g], width), 1)
        return columns == sides[firsts[g]:firsts[g] + sizes[g], 0:1].astype(jnp.int32)

    def weight_rows(q):
        owner = (x + q) % 2
        return pl.ds(pl.multiple_of(owner * feats, 128), feats)

    def pair_copy(g, k):
        return rcopy(plog.at[tok_of(1 + 2 * k), span(g)], pin.at[k, span(g)], p_send.at[g, k], p_recv.at[g, k], me_v, tok_of(1))

    def cross_copy(g):
        return rcopy(xo.at[span(g)], xi.at[span(g)], c_send.at[g], c_recv.at[g], me_v, tok_of(2))

    def stat_copy(g, k):
        return rcopy(stats_out.at[g], stats_in.at[g, me_v], s_send.at[g, k], s_recv.at[g, me_v], (me_v + k) % nv, me_t)

    def grad_copy(g, i):
        t = tok_of(2) if i == 2 else me_t
        return rcopy(dl.at[t, span(g)], dl.at[t, span(g)], d_send.at[g, i], d_recv.at[g, i], me_v, tok_of(2 if i == 0 else 1))

    def mix_copy(g, t):
        return rcopy(mix_out.at[t, span(g)], mix_in.at[t, span(g)], m_send.at[g, t], m_recv.at[g, t], other_x, me_t)

    def pass_copy(g, t):
        return rcopy(eo.at[t, span(g)], tin.at[c, span(g)], e_send.at[g, t], t_recv.at[g, c], me_v, t)

    def near_copy(g, t):
        return rcopy(eo.at[t, span(g)], fin.at[z, span(g)], e_send.at[g, t], f_recv.at[g, z], me_v, t)

    def far_copy(g, t):
        return rcopy(eo.at[t, span(g)], fin.at[z, span(g)], e_send.at[g, t], f_recv.at[g, z], me_t * 2 + x, t)

    def relay_copy(g, cc):
        return rcopy(tin.at[cc, span(g)], fin.at[z, span(g)], r_send.at[g, cc], f_recv.at[g, z], ((1 - y) * 2 + cc) * 2 + x, me_t)

    tile = 256

    def passed(g):
        @pl.when(is_inner)
        def _():
            for i in range(2):
                rcopy(
                    hid.at[span(g)], land.at[i, span(g)], a_send.at[g, 1], n_recv.at[g, i], landing(i) * 2 + x, me_t
                ).wait_recv()
                n_out(g, i).start()

                @pl.when(landing(i) != me_t)
                def _():
                    n_near(g, i).start()

                @pl.when(landing(i) == me_t)
                def _():
                    n_own(g, i).start()
                    hb[0, me_t, span(g)] = land[i, span(g)]

    def spread(g):
        @pl.when(home)
        def _():
            hb[0, me_t, span(g)] = hid[span(g)]

        for t in range(4):
            @pl.when(jnp.logical_not((home | landed) & (me_t == t)))
            def _():
                a_copy_in = rcopy(hid.at[span(g)], hb.at[0, t, span(g)], a_send.at[g, 0], a_recv.at[g, t], me_v, t)
                a_copy_in.wait_recv()
                x_copy(g, t).start()

    def logits_of(g):
        if g == 0:
            weights.wait()
        for t in range(4):
            x_copy(g, t).wait_recv()

        @pl.loop(0, width // tile)
        def _(j):
            cols = pl.ds(pl.multiple_of(j * tile, tile), tile)
            total = None
            for q in range(2):
                lhs = hb[q, :, span(g), :].reshape(4 * sizes[g], feats)
                term = jnp.dot(lhs, wbuf[weight_rows(q), cols], preferred_element_type=F32)
                total = term if total is None else total + term
            plog[:, span(g), cols] = total.reshape(4, sizes[g], tile)

        pair_copy(g, 1).start()
        pair_copy(g, 0).start()

    def cross_over(g):
        pair_copy(g, 1).wait_recv()
        value = plog[tok_of(2), span(g), :] + pin[1, span(g), :]
        top_of = jnp.max(jnp.abs(value), axis=1, keepdims=True)
        power = jnp.ceil(jnp.log2(jnp.maximum(top_of, jnp.float32(1e-20))) + jnp.float32(0.001))
        coded = jnp.round(value * jnp.exp2(15.0 - power)).astype(jnp.int32)
        xo[span(g), 0:width] = coded.astype(I16)
        xo[span(g), width:width + EXTRA] = jnp.broadcast_to(power.astype(jnp.int32), (sizes[g], EXTRA)).astype(I16)
        cross_copy(g).start()

    def softmax_of(g):
        pair_copy(g, 0).wait_recv()
        near_half = plog[me_t, span(g), :] + pin[0, span(g), :]
        cross_copy(g).wait_recv()
        power = xi[span(g), width:width + EXTRA].astype(jnp.int32).astype(F32)[:, 0:1]
        logits = near_half + xi[span(g), 0:width].astype(jnp.int32).astype(F32) * jnp.exp2(power - 15.0)
        masked = jnp.where(mask_ref[...] == 1, logits, jnp.float32(-1e30))
        local_max = jnp.max(masked, axis=1, keepdims=True)
        local_target = jnp.sum(jnp.where(onehot_of(g), logits, 0.0), axis=1, keepdims=True)
        local_sum = jnp.sum(jnp.exp(masked - local_max), axis=1, keepdims=True)
        m = sizes[g]
        lanes = lax.broadcasted_iota(jnp.int32, (m, 128), 1)
        packed = jnp.where(lanes == 0, local_max, jnp.where(lanes == 1, local_sum, local_target))
        if m < 128:
            packed = jnp.concatenate([packed, jnp.zeros((128 - m, 128), F32)], axis=0)
        mine = jnp.transpose(packed)[0:8]
        stats_out[g] = mine
        stats_in[g, me_v] = mine
        msk[span(g), :] = masked
        for k in range(1, nv):
            stat_copy(g, k).start()

    def grads_of(g):
        for k in range(1, nv):
            source = (me_v + nv - k) % nv
            rcopy(stats_out.at[g], stats_in.at[g, source], s_send.at[g, k], s_recv.at[g, source], source, me_t).wait_recv()
        row_max = stats_in[g, 0][0:1]
        for v in range(1, nv):
            row_max = jnp.maximum(row_max, stats_in[g, v][0:1])
        denominator = jnp.zeros_like(row_max)
        target_logit = jnp.zeros_like(row_max)
        for v in range(nv):
            got = stats_in[g, v]
            denominator += got[1:2] * jnp.exp(got[0:1] - row_max)
            target_logit += got[2:3]
        log_norm = row_max + jnp.log(denominator)
        loss_rows[g] = log_norm - target_logit
        column = jnp.transpose(jnp.broadcast_to(log_norm, (128, 128)))[0:sizes[g], 0:1]
        probabilities = jnp.exp(msk[span(g), :] - column)
        tok_grad = sides[firsts[g]:firsts[g] + sizes[g], 1:2]
        dl[me_t, span(g), :] = (tok_grad * (probabilities - onehot_of(g).astype(F32))).astype(BF)
        grad_copy(g, 0).start()
        grad_copy(g, 1).start()

    def grads_on(g):
        t = tok_of(2)
        rcopy(dl.at[t, span(g)], dl.at[t, span(g)], d_send.at[g, 0], d_recv.at[g, 0], me_v, t).wait_recv()
        grad_copy(g, 2).start()

    def terms_of(g):
        for i, r in ((1, 1), (2, 3)):
            t = tok_of(r)
            rcopy(dl.at[t, span(g)], dl.at[t, span(g)], d_send.at[g, i], d_recv.at[g, i], me_v, tok_of(1)).wait_recv()
        lhs = dl[:, span(g), :].reshape(4 * sizes[g], width)
        for q in (1, 0):
            value = lax.dot_general(
                lhs, wbuf[weight_rows(q), :], (((1,), (1,)), ((), ())), preferred_element_type=F32
            ).reshape(4, sizes[g], feats)
            if q == 0:
                near[:, span(g), :] = value
            else:
                mix_out[:, span(g), :] = value.astype(BF)
                for r in (2, 3, 1, 0):
                    mix_copy(g, tok_of(r)).start()

    def mixed(g, r):
        t = tok_of(r)
        mix_copy(g, t).wait_recv()
        both = (near[t, span(g), :] + mix_in[t, span(g), :].astype(F32)).astype(BF)
        if r == 0:
            @pl.when(home)
            def _():
                fin[z, span(g), :] = both

            @pl.when(jnp.logical_not(home))
            def _():
                eo[t, span(g), :] = both
                far_copy(g, t).start()
        elif r == 1:
            eo[t, span(g), :] = both
            far_copy(g, t).start()
        else:
            eo[t, span(g), :] = both

            @pl.when(home)
            def _():
                near_copy(g, t).start()

            @pl.when(jnp.logical_not(home))
            def _():
                pass_copy(g, t).start()

    def relayed(g, r):
        cc = (c + r) % 2

        @pl.when((1 - y) * 2 + cc != z)
        def _():
            rcopy(eo.at[0, span(g)], tin.at[cc, span(g)], e_send.at[g, 0], t_recv.at[g, cc], me_v, (1 - y) * 2 + cc).wait_recv()
            relay_copy(g, cc).start()

    def finish(g):
        total = None
        for zz in range(4):
            @pl.when(jnp.logical_not(home & (z == zz)))
            def _():
                rcopy(eo.at[0, span(g)], fin.at[zz, span(g)], e_send.at[g, 0], f_recv.at[g, zz], zz * 2 + x, me_t).wait_recv()
        for zz in range(4):
            term = fin[zz, span(g), :].astype(F32)
            total = term if total is None else total + term
        out_ref[span(g), :] = total.astype(BF)

    steps = {
        "ga": gather, "ld": passed, "sp": spread, "lg": logits_of, "co": cross_over, "sm": softmax_of, "gr": grads_of, "go": grads_on,
        "tm": terms_of, "fi": finish,
    }
    for r in range(4):
        steps[f"m{r}"] = lambda g, r=r: mixed(g, r)
    for r in range(2):
        steps[f"r{r}"] = lambda g, r=r: relayed(g, r)
    for item in PLAN:
        steps[item[:2]](int(item[2:]))

    loss_ref[...] = jnp.concatenate([loss_rows[g][:, 0:sizes[g]] for g in range(groups)], axis=1)

    for g in range(groups):
        a_copy(g).wait_send()
        n_copy(g).wait_send()

        @pl.when(jnp.logical_not(home))
        def _():
            o_copy(g).wait_send()

        @pl.when(is_inner)
        def _():
            for i in range(2):
                n_out(g, i).wait_send()

                @pl.when(landing(i) != me_t)
                def _():
                    n_near(g, i).wait_send()

        for t in range(4):
            x_copy(g, t).wait_send()
            mix_copy(g, t).wait_send()

            @pl.when(jnp.logical_not(home & (me_t == t)))
            def _():
                pass_copy(g, t).wait_send()

        for k in range(2):
            pair_copy(g, k).wait_send()

            @pl.when((1 - y) * 2 + k != z)
            def _():
                relay_copy(g, k).wait_send()

        cross_copy(g).wait_send()
        for k in range(1, nv):
            stat_copy(g, k).wait_send()
        for i in range(3):
            grad_copy(g, i).wait_send()


def fused(vocab_size, tok_size):
    def on_device(hidden, head_weight, targets, vocab_mask, token_grad):
        rows, feats = hidden.shape
        width = head_weight.shape[1]
        groups = len(SIZES)
        dma = pltpu.SemaphoreType.DMA
        vmem = pl.BlockSpec(memory_space=pltpu.VMEM)
        hbm = pl.BlockSpec(memory_space=pltpu.HBM)
        hidden_grad, loss = pl.pallas_call(
            lambda *refs: kernel(SIZES, *refs),
            out_shape=(
                jax.ShapeDtypeStruct((rows, feats), BF),
                jax.ShapeDtypeStruct((1, rows), F32),
            ),
            in_specs=[hbm, hbm] + [vmem] * 3,
            out_specs=(vmem, vmem),
            scratch_shapes=[
                pltpu.VMEM((rows, feats), BF),
                pltpu.VMEM((2 * feats, width), BF),
                pltpu.VMEM((2, rows, feats), BF),
                pltpu.VMEM((2, 4, rows, feats), BF),
                pltpu.VMEM((4, rows, width), F32),
                pltpu.VMEM((2, rows, width), F32),
                pltpu.VMEM((rows, width + EXTRA), I16),
                pltpu.VMEM((rows, width + EXTRA), I16),
                pltpu.VMEM((rows, width), F32),
                pltpu.VMEM((groups, 8, 128), F32),
                pltpu.VMEM((groups, vocab_size, 8, 128), F32),
                pltpu.VMEM((groups, 1, 128), F32),
                pltpu.VMEM((4, rows, width), BF),
                pltpu.VMEM((4, rows, feats), BF),
                pltpu.VMEM((4, rows, feats), BF),
                pltpu.VMEM((4, rows, feats), F32),
                pltpu.VMEM((4, rows, feats), BF),
                pltpu.VMEM((2, rows, feats), BF),
                pltpu.VMEM((4, rows, feats), BF),
                dma((groups,)), dma,
                dma((groups, 3)), dma((groups, 4)), dma((groups, 2)), dma((groups, 2, 2)), dma((groups, 4)), dma((groups, 4)),
                dma((groups, 2)), dma((groups, 2)), dma((groups,)), dma((groups,)),
                dma((groups, 8)), dma((groups, 8)), dma((groups, 3)), dma((groups, 3)),
                dma((groups, 4)), dma((groups, 4)), dma((groups, 4)), dma((groups, 4)),
                dma((groups, 2)), dma((groups, 2)),
            ],
            compiler_params=pltpu.CompilerParams(
                collective_id=0, has_side_effects=True, vmem_limit_bytes=60 * 1024 * 1024
            ),
        )(hidden, head_weight, targets[None, :], vocab_mask[None, :], token_grad[None, :])
        return (hidden_grad, loss.reshape(rows))

    return on_device


def solution(mesh):
    placed = (P("tok", "vocab"), P("tok", "vocab"), P("tok"), P("vocab"), P("tok"))
    vocab_size, tok_size = mesh.shape["vocab"], mesh.shape["tok"]

    def body(hidden, head_weight, *rest):
        rows, feats = hidden.shape
        fits = tok_size == 4 and vocab_size == 8 and feats % 128 == 0 and head_weight.shape[1] % 256 == 0
        fits = fits and rows <= 256 and rows == sum(SIZES)
        build = fused if fits else make_on_device
        return build(vocab_size, tok_size)(hidden, head_weight, *rest)

    return jax.shard_map(
        body,
        mesh=mesh,
        in_specs=placed,
        out_specs=(P("tok", "vocab"), P("tok")),
        check_vma=False,
    )
```

```python
import jax
import jax.numpy as jnp
from jax import lax
from jax.experimental import pallas as pl
from jax.experimental.pallas import tpu as pltpu
from jax.sharding import PartitionSpec as P


def make_on_device(vocab_size, tok_size):
    share = vocab_size // tok_size
    moves = [
        (b * tok_size + a, (a * share + b % share) * tok_size + b // share)
        for a in range(tok_size)
        for b in range(vocab_size)
    ]
    back = [(there, here) for here, there in moves]

    def on_device(hidden, head_weight, targets, vocab_mask, token_grad):
        rows, feats = hidden.shape
        block_width = head_weight.shape[1]
        moved = lax.ppermute(hidden, ("vocab", "tok"), moves)
        pieces = lax.all_gather(moved, "vocab")
        gathered = (
            pieces.reshape(tok_size, share, rows, feats)
            .transpose(0, 2, 1, 3)
            .reshape(tok_size * rows, share * feats)
        )
        partial_logits = jnp.dot(gathered, head_weight, preferred_element_type=jnp.float32)
        logits = lax.psum_scatter(partial_logits, "tok", scatter_dimension=0, tiled=True)
        first_column = lax.axis_index("vocab") * block_width
        masked = jnp.where(vocab_mask[None, :] == 1, logits, jnp.float32(-1e30))
        local_max = jnp.max(masked, axis=1)
        columns = first_column + jnp.arange(block_width, dtype=jnp.int32)
        onehot = columns[None, :] == targets[:, None]
        local_target = jnp.sum(jnp.where(onehot, logits, jnp.float32(0.0)), axis=1)
        weights = jnp.exp(masked - local_max[:, None])
        local_sum = jnp.sum(weights, axis=1)
        stats = lax.all_gather(jnp.stack([local_max, local_sum, local_target]), "vocab")
        row_max = jnp.max(stats[:, 0], axis=0)
        denominator = jnp.sum(stats[:, 1] * jnp.exp(stats[:, 0] - row_max[None]), axis=0)
        target_logit = jnp.sum(stats[:, 2], axis=0)
        log_norm = row_max + jnp.log(denominator)
        token_loss = log_norm - target_logit
        probabilities = jnp.exp(masked - log_norm[:, None])
        logit_grad = (
            token_grad[:, None] * (probabilities - onehot.astype(jnp.float32))
        ).astype(jnp.bfloat16)
        all_grads = lax.all_gather(logit_grad, "tok", axis=0, tiled=True)
        partial_value = lax.dot_general(
            all_grads,
            head_weight,
            (((1,), (1,)), ((), ())),
            preferred_element_type=jnp.float32,
        )
        blocks = (
            partial_value.reshape(tok_size, rows, share, feats)
            .transpose(0, 2, 1, 3)
            .reshape(vocab_size, rows, feats)
        )
        summed = lax.psum_scatter(blocks, "vocab", scatter_dimension=0, tiled=False)
        hidden_grad = lax.ppermute(summed.astype(jnp.bfloat16), ("vocab", "tok"), back)
        return (hidden_grad, token_loss)

    return on_device


SIZES = (48, 48, 48, 48)
EXTRA = 128
BF = jnp.bfloat16
F32 = jnp.float32
I16 = jnp.int16


PLAN = (
    "ga0", "ld0", "ga1", "sp0", "ld1", "ga2", "sp1", "ld2", "lg0", "ga3", "co0", "sp2", "sm0", "ld3", "lg1",
    "co1", "sp3", "gr0", "sm1", "lg2", "go0", "co2", "tm0", "gr1", "lg3", "co3", "sm2", "go1", "m20", "tm1",
    "m30", "m10", "sm3", "r00", "gr2", "r10", "m00", "m31", "m21", "go2", "tm2", "r11", "m11", "gr3", "go3",
    "m01", "r01", "m32", "tm3", "m12", "m22", "r12", "fi1", "m23", "fi0", "m02", "m33", "r02", "m13", "m03",
    "r03", "fi2", "r13", "fi3",
)


def kernel(
    sizes,
    hidden_ref, weight_ref, targets_ref, mask_ref, grad_ref,
    out_ref, loss_ref,
    hid, wbuf, land, hb, plog, pin, xo, xi, msk, stats_out, stats_in, loss_rows, dl,
    mix_out, mix_in, near, eo, tin, fin,
    l_sem, w_sem, a_send, a_recv, n_recv, n_send, x_send, x_recv, p_send, p_recv, c_send, c_recv,
    s_send, s_recv, d_send, d_recv, m_send, m_recv, e_send, f_recv, t_recv, r_send,
):
    rows, feats = hidden_ref.shape
    groups = len(sizes)
    firsts = [sum(sizes[:g]) for g in range(groups)]
    width = weight_ref.shape[1]
    me_v = lax.axis_index("vocab")
    me_t = lax.axis_index("tok")
    z, x = me_v // 2, me_v % 2
    y, c = me_t // 2, me_t % 2
    nv = 8

    def dev(v, t):
        return {"vocab": v, "tok": t}

    def tok_of(r):
        return ((y + r // 2) % 2) * 2 + (c + r % 2) % 2

    other_x = z * 2 + (1 - x)

    def rcopy(src, dst, ss, rs, v, t):
        return pltpu.make_async_remote_copy(
            src_ref=src, dst_ref=dst, send_sem=ss, recv_sem=rs,
            device_id=dev(v, t), device_id_type=pl.DeviceIdType.MESH,
        )

    def span(g):
        return pl.ds(firsts[g], sizes[g])

    loads = [pltpu.make_async_copy(hidden_ref.at[span(g)], hid.at[span(g)], l_sem.at[g]) for g in range(groups)]
    for load in loads:
        load.start()
    weights = pltpu.make_async_copy(weight_ref, wbuf, w_sem)
    weights.start()

    barrier = pltpu.get_barrier_semaphore()
    for k in range(4):
        for r in range(4):
            if k or r:
                pl.semaphore_signal(
                    barrier, inc=1, device_id=dev(((z + k) % 4) * 2 + x, tok_of(r)), device_id_type=pl.DeviceIdType.MESH
                )
        pl.semaphore_signal(
            barrier, inc=1, device_id=dev(((z + k) % 4) * 2 + 1 - x, me_t), device_id_type=pl.DeviceIdType.MESH
        )
    pl.semaphore_wait(barrier, 19)

    home = me_t == z

    side = z // 2
    partner = z + 1 - 2 * (z % 2)
    inner = jnp.where(z < 2, 2, 1)
    outer = jnp.where(z < 2, 0, 3)
    is_inner = (z == 1) | (z == 2)
    landed = is_inner & (me_t // 2 == 1 - side)

    def a_copy(g):
        return rcopy(hid.at[span(g)], hb.at[0, me_t, span(g)], a_send.at[g, 0], a_recv.at[g, me_t], partner * 2 + x, z)

    def n_copy(g):
        i = jnp.where(is_inner, 0, 1)
        return rcopy(hid.at[span(g)], land.at[i, span(g)], a_send.at[g, 1], n_recv.at[g, i], inner * 2 + x, me_t)

    def o_copy(g):
        return rcopy(hid.at[span(g)], hb.at[0, me_t, span(g)], a_send.at[g, 2], a_recv.at[g, me_t], me_v, z)

    def landing(i):
        return jnp.where(z == 2, 1 - i, 2 + i)

    def n_out(g, i):
        return rcopy(
            land.at[i, span(g)], hb.at[0, me_t, span(g)], n_send.at[g, i, 0], a_recv.at[g, me_t], outer * 2 + x, landing(i)
        )

    def n_near(g, i):
        return rcopy(land.at[i, span(g)], hb.at[0, me_t, span(g)], n_send.at[g, i, 1], a_recv.at[g, me_t], me_v, landing(i))

    def n_own(g, i):
        return rcopy(land.at[i, span(g)], hb.at[1, me_t, span(g)], x_send.at[g, me_t], x_recv.at[g, me_t], other_x, me_t)

    def x_copy(g, t):
        return rcopy(hb.at[0, t, span(g)], hb.at[1, t, span(g)], x_send.at[g, t], x_recv.at[g, t], other_x, me_t)

    def x_own(g):
        return rcopy(hid.at[span(g)], hb.at[1, me_t, span(g)], x_send.at[g, me_t], x_recv.at[g, me_t], other_x, me_t)

    def gather(g):
        loads[g].wait()
        a_copy(g).start()
        n_copy(g).start()

        @pl.when(jnp.logical_not(home))
        def _():
            o_copy(g).start()

        @pl.when(home)
        def _():
            x_own(g).start()


    top = jnp.concatenate([targets_ref[...].astype(F32), grad_ref[...]], axis=0)
    top = jnp.concatenate([top, jnp.zeros((2, 256 - rows), F32)], axis=1)
    sides = jnp.transpose(jnp.concatenate([top, jnp.zeros((126, 256), F32)], axis=0))

    def onehot_of(g):
        columns = me_v * width + lax.broadcasted_iota(jnp.int32, (sizes[g], width), 1)
        return columns == sides[firsts[g]:firsts[g] + sizes[g], 0:1].astype(jnp.int32)

    def weight_rows(q):
        owner = (x + q) % 2
        return pl.ds(pl.multiple_of(owner * feats, 128), feats)

    def pair_copy(g, k):
        return rcopy(plog.at[tok_of(1 + 2 * k), span(g)], pin.at[k, span(g)], p_send.at[g, k], p_recv.at[g, k], me_v, tok_of(1))

    def cross_copy(g):
        return rcopy(xo.at[span(g)], xi.at[span(g)], c_send.at[g], c_recv.at[g], me_v, tok_of(2))

    def stat_copy(g, k):
        return rcopy(stats_out.at[g], stats_in.at[g, me_v], s_send.at[g, k], s_recv.at[g, me_v], (me_v + k) % nv, me_t)

    def grad_copy(g, i):
        t = tok_of(2) if i == 2 else me_t
        return rcopy(dl.at[t, span(g)], dl.at[t, span(g)], d_send.at[g, i], d_recv.at[g, i], me_v, tok_of(2 if i == 0 else 1))

    def mix_copy(g, t):
        return rcopy(mix_out.at[t, span(g)], mix_in.at[t, span(g)], m_send.at[g, t], m_recv.at[g, t], other_x, me_t)

    def pass_copy(g, t):
        return rcopy(eo.at[t, span(g)], tin.at[c, span(g)], e_send.at[g, t], t_recv.at[g, c], me_v, t)

    def near_copy(g, t):
        return rcopy(eo.at[t, span(g)], fin.at[z, span(g)], e_send.at[g, t], f_recv.at[g, z], me_v, t)

    def far_copy(g, t):
        return rcopy(eo.at[t, span(g)], fin.at[z, span(g)], e_send.at[g, t], f_recv.at[g, z], me_t * 2 + x, t)

    def relay_copy(g, cc):
        return rcopy(tin.at[cc, span(g)], fin.at[z, span(g)], r_send.at[g, cc], f_recv.at[g, z], ((1 - y) * 2 + cc) * 2 + x, me_t)

    tile = 256

    def passed(g):
        @pl.when(is_inner)
        def _():
            for i in range(2):
                rcopy(
                    hid.at[span(g)], land.at[i, span(g)], a_send.at[g, 1], n_recv.at[g, i], landing(i) * 2 + x, me_t
                ).wait_recv()
                n_out(g, i).start()

                @pl.when(landing(i) != me_t)
                def _():
                    n_near(g, i).start()

                @pl.when(landing(i) == me_t)
                def _():
                    n_own(g, i).start()
                    hb[0, me_t, span(g)] = land[i, span(g)]

    def spread(g):
        @pl.when(home)
        def _():
            hb[0, me_t, span(g)] = hid[span(g)]

        for t in range(4):
            @pl.when(jnp.logical_not((home | landed) & (me_t == t)))
            def _():
                a_copy_in = rcopy(hid.at[span(g)], hb.at[0, t, span(g)], a_send.at[g, 0], a_recv.at[g, t], me_v, t)
                a_copy_in.wait_recv()
                x_copy(g, t).start()

    def logits_of(g):
        if g == 0:
            weights.wait()
        for t in range(4):
            x_copy(g, t).wait_recv()

        @pl.loop(0, width // tile)
        def _(j):
            cols = pl.ds(pl.multiple_of(j * tile, tile), tile)
            total = None
            for q in range(2):
                lhs = hb[q, :, span(g), :].reshape(4 * sizes[g], feats)
                term = jnp.dot(lhs, wbuf[weight_rows(q), cols], preferred_element_type=F32)
                total = term if total is None else total + term
            plog[:, span(g), cols] = total.reshape(4, sizes[g], tile)

        pair_copy(g, 1).start()
        pair_copy(g, 0).start()

    def cross_over(g):
        pair_copy(g, 1).wait_recv()
        value = plog[tok_of(2), span(g), :] + pin[1, span(g), :]
        top_of = jnp.max(jnp.abs(value), axis=1, keepdims=True)
        power = jnp.ceil(jnp.log2(jnp.maximum(top_of, jnp.float32(1e-20))) + jnp.float32(0.001))
        coded = jnp.round(value * jnp.exp2(15.0 - power)).astype(jnp.int32)
        xo[span(g), 0:width] = coded.astype(I16)
        xo[span(g), width:width + EXTRA] = jnp.broadcast_to(power.astype(jnp.int32), (sizes[g], EXTRA)).astype(I16)
        cross_copy(g).start()

    def softmax_of(g):
        pair_copy(g, 0).wait_recv()
        near_half = plog[me_t, span(g), :] + pin[0, span(g), :]
        cross_copy(g).wait_recv()
        power = xi[span(g), width:width + EXTRA].astype(jnp.int32).astype(F32)[:, 0:1]
        logits = near_half + xi[span(g), 0:width].astype(jnp.int32).astype(F32) * jnp.exp2(power - 15.0)
        masked = jnp.where(mask_ref[...] == 1, logits, jnp.float32(-1e30))
        local_max = jnp.max(masked, axis=1, keepdims=True)
        local_target = jnp.sum(jnp.where(onehot_of(g), logits, 0.0), axis=1, keepdims=True)
        local_sum = jnp.sum(jnp.exp(masked - local_max), axis=1, keepdims=True)
        m = sizes[g]
        lanes = lax.broadcasted_iota(jnp.int32, (m, 128), 1)
        packed = jnp.where(lanes == 0, local_max, jnp.where(lanes == 1, local_sum, local_target))
        if m < 128:
            packed = jnp.concatenate([packed, jnp.zeros((128 - m, 128), F32)], axis=0)
        mine = jnp.transpose(packed)[0:8]
        stats_out[g] = mine
        stats_in[g, me_v] = mine
        msk[span(g), :] = masked
        for k in range(1, nv):
            stat_copy(g, k).start()

    def grads_of(g):
        for k in range(1, nv):
            source = (me_v + nv - k) % nv
            rcopy(stats_out.at[g], stats_in.at[g, source], s_send.at[g, k], s_recv.at[g, source], source, me_t).wait_recv()
        row_max = stats_in[g, 0][0:1]
        for v in range(1, nv):
            row_max = jnp.maximum(row_max, stats_in[g, v][0:1])
        denominator = jnp.zeros_like(row_max)
        target_logit = jnp.zeros_like(row_max)
        for v in range(nv):
            got = stats_in[g, v]
            denominator += got[1:2] * jnp.exp(got[0:1] - row_max)
            target_logit += got[2:3]
        log_norm = row_max + jnp.log(denominator)
        loss_rows[g] = log_norm - target_logit
        column = jnp.transpose(jnp.broadcast_to(log_norm, (128, 128)))[0:sizes[g], 0:1]
        probabilities = jnp.exp(msk[span(g), :] - column)
        tok_grad = sides[firsts[g]:firsts[g] + sizes[g], 1:2]
        dl[me_t, span(g), :] = (tok_grad * (probabilities - onehot_of(g).astype(F32))).astype(BF)
        grad_copy(g, 0).start()
        grad_copy(g, 1).start()

    def grads_on(g):
        t = tok_of(2)
        rcopy(dl.at[t, span(g)], dl.at[t, span(g)], d_send.at[g, 0], d_recv.at[g, 0], me_v, t).wait_recv()
        grad_copy(g, 2).start()

    def terms_of(g):
        for i, r in ((1, 1), (2, 3)):
            t = tok_of(r)
            rcopy(dl.at[t, span(g)], dl.at[t, span(g)], d_send.at[g, i], d_recv.at[g, i], me_v, tok_of(1)).wait_recv()
        lhs = dl[:, span(g), :].reshape(4 * sizes[g], width)
        for q in (1, 0):
            value = lax.dot_general(
                lhs, wbuf[weight_rows(q), :], (((1,), (1,)), ((), ())), preferred_element_type=F32
            ).reshape(4, sizes[g], feats)
            if q == 0:
                near[:, span(g), :] = value
            else:
                mix_out[:, span(g), :] = value.astype(BF)
                for r in (2, 3, 1, 0):
                    mix_copy(g, tok_of(r)).start()

    def mixed(g, r):
        t = tok_of(r)
        mix_copy(g, t).wait_recv()
        both = (near[t, span(g), :] + mix_in[t, span(g), :].astype(F32)).astype(BF)
        if r == 0:
            @pl.when(home)
            def _():
                fin[z, span(g), :] = both

            @pl.when(jnp.logical_not(home))
            def _():
                eo[t, span(g), :] = both
                far_copy(g, t).start()
        elif r == 1:
            eo[t, span(g), :] = both
            far_copy(g, t).start()
        else:
            eo[t, span(g), :] = both

            @pl.when(home)
            def _():
                near_copy(g, t).start()

            @pl.when(jnp.logical_not(home))
            def _():
                pass_copy(g, t).start()

    def relayed(g, r):
        cc = (c + r) % 2

        @pl.when((1 - y) * 2 + cc != z)
        def _():
            rcopy(eo.at[0, span(g)], tin.at[cc, span(g)], e_send.at[g, 0], t_recv.at[g, cc], me_v, (1 - y) * 2 + cc).wait_recv()
            relay_copy(g, cc).start()

    def finish(g):
        total = None
        for zz in range(4):
            @pl.when(jnp.logical_not(home & (z == zz)))
            def _():
                rcopy(eo.at[0, span(g)], fin.at[zz, span(g)], e_send.at[g, 0], f_recv.at[g, zz], zz * 2 + x, me_t).wait_recv()
        for zz in range(4):
            term = fin[zz, span(g), :].astype(F32)
            total = term if total is None else total + term
        out_ref[span(g), :] = total.astype(BF)

    steps = {
        "ga": gather, "ld": passed, "sp": spread, "lg": logits_of, "co": cross_over, "sm": softmax_of, "gr": grads_of, "go": grads_on,
        "tm": terms_of, "fi": finish,
    }
    for r in range(4):
        steps[f"m{r}"] = lambda g, r=r: mixed(g, r)
    for r in range(2):
        steps[f"r{r}"] = lambda g, r=r: relayed(g, r)
    for item in PLAN:
        steps[item[:2]](int(item[2:]))

    loss_ref[...] = jnp.concatenate([loss_rows[g][:, 0:sizes[g]] for g in range(groups)], axis=1)

    for g in range(groups):
        a_copy(g).wait_send()
        n_copy(g).wait_send()

        @pl.when(jnp.logical_not(home))
        def _():
            o_copy(g).wait_send()

        @pl.when(is_inner)
        def _():
            for i in range(2):
                n_out(g, i).wait_send()

                @pl.when(landing(i) != me_t)
                def _():
                    n_near(g, i).wait_send()

        for t in range(4):
            x_copy(g, t).wait_send()
            mix_copy(g, t).wait_send()

            @pl.when(jnp.logical_not(home & (me_t == t)))
            def _():
                pass_copy(g, t).wait_send()

        for k in range(2):
            pair_copy(g, k).wait_send()

            @pl.when((1 - y) * 2 + k != z)
            def _():
                relay_copy(g, k).wait_send()

        cross_copy(g).wait_send()
        for k in range(1, nv):
            stat_copy(g, k).wait_send()
        for i in range(3):
            grad_copy(g, i).wait_send()


def fused(vocab_size, tok_size):
    def on_device(hidden, head_weight, targets, vocab_mask, token_grad):
        rows, feats = hidden.shape
        width = head_weight.shape[1]
        groups = len(SIZES)
        dma = pltpu.SemaphoreType.DMA
        vmem = pl.BlockSpec(memory_space=pltpu.VMEM)
        hbm = pl.BlockSpec(memory_space=pltpu.HBM)
        hidden_grad, loss = pl.pallas_call(
            lambda *refs: kernel(SIZES, *refs),
            out_shape=(
                jax.ShapeDtypeStruct((rows, feats), BF),
                jax.ShapeDtypeStruct((1, rows), F32),
            ),
            in_specs=[hbm, hbm] + [vmem] * 3,
            out_specs=(vmem, vmem),
            scratch_shapes=[
                pltpu.VMEM((rows, feats), BF),
                pltpu.VMEM((2 * feats, width), BF),
                pltpu.VMEM((2, rows, feats), BF),
                pltpu.VMEM((2, 4, rows, feats), BF),
                pltpu.VMEM((4, rows, width), F32),
                pltpu.VMEM((2, rows, width), F32),
                pltpu.VMEM((rows, width + EXTRA), I16),
                pltpu.VMEM((rows, width + EXTRA), I16),
                pltpu.VMEM((rows, width), F32),
                pltpu.VMEM((groups, 8, 128), F32),
                pltpu.VMEM((groups, vocab_size, 8, 128), F32),
                pltpu.VMEM((groups, 1, 128), F32),
                pltpu.VMEM((4, rows, width), BF),
                pltpu.VMEM((4, rows, feats), BF),
                pltpu.VMEM((4, rows, feats), BF),
                pltpu.VMEM((4, rows, feats), F32),
                pltpu.VMEM((4, rows, feats), BF),
                pltpu.VMEM((2, rows, feats), BF),
                pltpu.VMEM((4, rows, feats), BF),
                dma((groups,)), dma,
                dma((groups, 3)), dma((groups, 4)), dma((groups, 2)), dma((groups, 2, 2)), dma((groups, 4)), dma((groups, 4)),
                dma((groups, 2)), dma((groups, 2)), dma((groups,)), dma((groups,)),
                dma((groups, 8)), dma((groups, 8)), dma((groups, 3)), dma((groups, 3)),
                dma((groups, 4)), dma((groups, 4)), dma((groups, 4)), dma((groups, 4)),
                dma((groups, 2)), dma((groups, 2)),
            ],
            compiler_params=pltpu.CompilerParams(
                collective_id=0, has_side_effects=True, vmem_limit_bytes=60 * 1024 * 1024
            ),
        )(hidden, head_weight, targets[None, :], vocab_mask[None, :], token_grad[None, :])
        def hand_on(grad_ref, loss_ref, grad_out, loss_out, grad_buf, loss_buf, sem):
            ins = [
                pltpu.make_async_copy(loss_ref, loss_buf, sem.at[0]),
                pltpu.make_async_copy(grad_ref, grad_buf, sem.at[1]),
            ]
            outs = [
                pltpu.make_async_copy(loss_buf, loss_out, sem.at[2]),
                pltpu.make_async_copy(grad_buf, grad_out, sem.at[3]),
            ]
            for copy in ins:
                copy.start()
            for copy, after in zip(ins, outs):
                copy.wait()
                after.start()
            for copy in outs:
                copy.wait()

        hidden_grad, loss = pl.pallas_call(
            hand_on,
            out_shape=(
                jax.ShapeDtypeStruct((rows, feats), BF),
                jax.ShapeDtypeStruct((1, rows), F32),
            ),
            in_specs=[hbm, hbm],
            out_specs=(hbm, hbm),
            scratch_shapes=[pltpu.VMEM((rows, feats), BF), pltpu.VMEM((1, rows), F32), dma((4,))],
        )(hidden_grad, loss)
        return (hidden_grad, loss.reshape(rows))

    return on_device


def solution(mesh):
    placed = (P("tok", "vocab"), P("tok", "vocab"), P("tok"), P("vocab"), P("tok"))
    vocab_size, tok_size = mesh.shape["vocab"], mesh.shape["tok"]

    def body(hidden, head_weight, *rest):
        rows, feats = hidden.shape
        fits = tok_size == 4 and vocab_size == 8 and feats % 128 == 0 and head_weight.shape[1] % 256 == 0
        fits = fits and rows <= 256 and rows == sum(SIZES)
        build = fused if fits else make_on_device
        return build(vocab_size, tok_size)(hidden, head_weight, *rest)

    return jax.shard_map(
        body,
        mesh=mesh,
        in_specs=placed,
        out_specs=(P("tok", "vocab"), P("tok")),
        check_vma=False,
    )
```

```python
import jax
import jax.numpy as jnp
from jax import lax
from jax.experimental import pallas as pl
from jax.experimental.pallas import tpu as pltpu
from jax.sharding import PartitionSpec as P


def make_on_device(vocab_size, tok_size):
    share = vocab_size // tok_size
    moves = [
        (b * tok_size + a, (a * share + b % share) * tok_size + b // share)
        for a in range(tok_size)
        for b in range(vocab_size)
    ]
    back = [(there, here) for here, there in moves]

    def on_device(hidden, head_weight, targets, vocab_mask, token_grad):
        rows, feats = hidden.shape
        block_width = head_weight.shape[1]
        moved = lax.ppermute(hidden, ("vocab", "tok"), moves)
        pieces = lax.all_gather(moved, "vocab")
        gathered = (
            pieces.reshape(tok_size, share, rows, feats)
            .transpose(0, 2, 1, 3)
            .reshape(tok_size * rows, share * feats)
        )
        partial_logits = jnp.dot(gathered, head_weight, preferred_element_type=jnp.float32)
        logits = lax.psum_scatter(partial_logits, "tok", scatter_dimension=0, tiled=True)
        first_column = lax.axis_index("vocab") * block_width
        masked = jnp.where(vocab_mask[None, :] == 1, logits, jnp.float32(-1e30))
        local_max = jnp.max(masked, axis=1)
        columns = first_column + jnp.arange(block_width, dtype=jnp.int32)
        onehot = columns[None, :] == targets[:, None]
        local_target = jnp.sum(jnp.where(onehot, logits, jnp.float32(0.0)), axis=1)
        weights = jnp.exp(masked - local_max[:, None])
        local_sum = jnp.sum(weights, axis=1)
        stats = lax.all_gather(jnp.stack([local_max, local_sum, local_target]), "vocab")
        row_max = jnp.max(stats[:, 0], axis=0)
        denominator = jnp.sum(stats[:, 1] * jnp.exp(stats[:, 0] - row_max[None]), axis=0)
        target_logit = jnp.sum(stats[:, 2], axis=0)
        log_norm = row_max + jnp.log(denominator)
        token_loss = log_norm - target_logit
        probabilities = jnp.exp(masked - log_norm[:, None])
        logit_grad = (
            token_grad[:, None] * (probabilities - onehot.astype(jnp.float32))
        ).astype(jnp.bfloat16)
        all_grads = lax.all_gather(logit_grad, "tok", axis=0, tiled=True)
        partial_value = lax.dot_general(
            all_grads,
            head_weight,
            (((1,), (1,)), ((), ())),
            preferred_element_type=jnp.float32,
        )
        blocks = (
            partial_value.reshape(tok_size, rows, share, feats)
            .transpose(0, 2, 1, 3)
            .reshape(vocab_size, rows, feats)
        )
        summed = lax.psum_scatter(blocks, "vocab", scatter_dimension=0, tiled=False)
        hidden_grad = lax.ppermute(summed.astype(jnp.bfloat16), ("vocab", "tok"), back)
        return (hidden_grad, token_loss)

    return on_device


SIZES = (48, 48, 48, 48)
EXTRA = 128
BF = jnp.bfloat16
F32 = jnp.float32
I16 = jnp.int16


PLAN = (
    "ga0", "ld0", "ga1", "sp0", "ld1", "ga2", "sp1", "ld2", "lg0", "ga3", "co0", "sp2", "sm0", "ld3", "lg1",
    "co1", "sp3", "gr0", "lg2", "sm1", "co2", "go0", "tm0", "gr1", "lg3", "m20", "sm2", "go1", "co3", "m30",
    "r00", "tm1", "m10", "gr2", "sm3", "r10", "m21", "go2", "m00", "m31", "tm2", "m11", "r01", "gr3", "m01",
    "m22", "r11", "m32", "go3", "r02", "fi0", "tm3", "m12", "r12", "m23", "m02", "m33", "m13", "m03", "r03",
    "r13", "fi2", "fi1", "fi3",
)


def kernel(
    sizes,
    hidden_ref, weight_ref, targets_ref, mask_ref, grad_ref,
    out_ref, loss_ref,
    hid, wbuf, land, hb, plog, pin, xo, xi, msk, stats_out, stats_in, loss_rows, dl,
    mix_out, mix_in, near, eo, tin, fin,
    l_sem, w_sem, a_send, a_recv, n_recv, n_send, x_send, x_recv, p_send, p_recv, c_send, c_recv,
    s_send, s_recv, d_send, d_recv, m_send, m_recv, e_send, f_recv, t_recv, r_send,
):
    rows, feats = hidden_ref.shape
    groups = len(sizes)
    firsts = [sum(sizes[:g]) for g in range(groups)]
    width = weight_ref.shape[1]
    me_v = lax.axis_index("vocab")
    me_t = lax.axis_index("tok")
    z, x = me_v // 2, me_v % 2
    y, c = me_t // 2, me_t % 2
    nv = 8

    def dev(v, t):
        return {"vocab": v, "tok": t}

    def tok_of(r):
        return ((y + r // 2) % 2) * 2 + (c + r % 2) % 2

    other_x = z * 2 + (1 - x)

    def rcopy(src, dst, ss, rs, v, t):
        return pltpu.make_async_remote_copy(
            src_ref=src, dst_ref=dst, send_sem=ss, recv_sem=rs,
            device_id=dev(v, t), device_id_type=pl.DeviceIdType.MESH,
        )

    def span(g):
        return pl.ds(firsts[g], sizes[g])

    loads = [pltpu.make_async_copy(hidden_ref.at[span(g)], hid.at[span(g)], l_sem.at[g]) for g in range(groups)]
    for load in loads:
        load.start()
    weights = pltpu.make_async_copy(weight_ref, wbuf, w_sem)
    weights.start()

    barrier = pltpu.get_barrier_semaphore()
    for k in range(4):
        for r in range(4):
            if k or r:
                pl.semaphore_signal(
                    barrier, inc=1, device_id=dev(((z + k) % 4) * 2 + x, tok_of(r)), device_id_type=pl.DeviceIdType.MESH
                )
        pl.semaphore_signal(
            barrier, inc=1, device_id=dev(((z + k) % 4) * 2 + 1 - x, me_t), device_id_type=pl.DeviceIdType.MESH
        )
    pl.semaphore_wait(barrier, 19)

    home = me_t == z

    side = z // 2
    partner = z + 1 - 2 * (z % 2)
    inner = jnp.where(z < 2, 2, 1)
    outer = jnp.where(z < 2, 0, 3)
    is_inner = (z == 1) | (z == 2)
    landed = is_inner & (me_t // 2 == 1 - side)

    def a_copy(g):
        return rcopy(hid.at[span(g)], hb.at[0, me_t, span(g)], a_send.at[g, 0], a_recv.at[g, me_t], partner * 2 + x, z)

    def n_copy(g):
        i = jnp.where(is_inner, 0, 1)
        return rcopy(hid.at[span(g)], land.at[i, span(g)], a_send.at[g, 1], n_recv.at[g, i], inner * 2 + x, me_t)

    def o_copy(g):
        return rcopy(hid.at[span(g)], hb.at[0, me_t, span(g)], a_send.at[g, 2], a_recv.at[g, me_t], me_v, z)

    def landing(i):
        return jnp.where(z == 2, 1 - i, 2 + i)

    def n_out(g, i):
        return rcopy(
            land.at[i, span(g)], hb.at[0, me_t, span(g)], n_send.at[g, i, 0], a_recv.at[g, me_t], outer * 2 + x, landing(i)
        )

    def n_near(g, i):
        return rcopy(land.at[i, span(g)], hb.at[0, me_t, span(g)], n_send.at[g, i, 1], a_recv.at[g, me_t], me_v, landing(i))

    def n_own(g, i):
        return rcopy(land.at[i, span(g)], hb.at[1, me_t, span(g)], x_send.at[g, me_t], x_recv.at[g, me_t], other_x, me_t)

    def x_copy(g, t):
        return rcopy(hb.at[0, t, span(g)], hb.at[1, t, span(g)], x_send.at[g, t], x_recv.at[g, t], other_x, me_t)

    def x_own(g):
        return rcopy(hid.at[span(g)], hb.at[1, me_t, span(g)], x_send.at[g, me_t], x_recv.at[g, me_t], other_x, me_t)

    def gather(g):
        loads[g].wait()
        a_copy(g).start()
        n_copy(g).start()

        @pl.when(jnp.logical_not(home))
        def _():
            o_copy(g).start()

        @pl.when(home)
        def _():
            x_own(g).start()


    top = jnp.concatenate([targets_ref[...].astype(F32), grad_ref[...]], axis=0)
    top = jnp.concatenate([top, jnp.zeros((2, 256 - rows), F32)], axis=1)
    sides = jnp.transpose(jnp.concatenate([top, jnp.zeros((126, 256), F32)], axis=0))

    def onehot_of(g):
        columns = me_v * width + lax.broadcasted_iota(jnp.int32, (sizes[g], width), 1)
        return columns == sides[firsts[g]:firsts[g] + sizes[g], 0:1].astype(jnp.int32)

    def weight_rows(q):
        owner = (x + q) % 2
        return pl.ds(pl.multiple_of(owner * feats, 128), feats)

    def pair_copy(g, k):
        return rcopy(plog.at[tok_of(1 + 2 * k), span(g)], pin.at[k, span(g)], p_send.at[g, k], p_recv.at[g, k], me_v, tok_of(1))

    def cross_copy(g):
        return rcopy(xo.at[span(g)], xi.at[span(g)], c_send.at[g], c_recv.at[g], me_v, tok_of(2))

    def stat_copy(g, k):
        return rcopy(stats_out.at[g], stats_in.at[g, me_v], s_send.at[g, k], s_recv.at[g, me_v], (me_v + k) % nv, me_t)

    def grad_copy(g, i):
        t = tok_of(2) if i == 2 else me_t
        return rcopy(dl.at[t, span(g)], dl.at[t, span(g)], d_send.at[g, i], d_recv.at[g, i], me_v, tok_of(2 if i == 0 else 1))

    def mix_copy(g, t):
        return rcopy(mix_out.at[t, span(g)], mix_in.at[t, span(g)], m_send.at[g, t], m_recv.at[g, t], other_x, me_t)

    def pass_copy(g, t):
        return rcopy(eo.at[t, span(g)], tin.at[c, span(g)], e_send.at[g, t], t_recv.at[g, c], me_v, t)

    def near_copy(g, t):
        return rcopy(eo.at[t, span(g)], fin.at[z, span(g)], e_send.at[g, t], f_recv.at[g, z], me_v, t)

    def far_copy(g, t):
        return rcopy(eo.at[t, span(g)], fin.at[z, span(g)], e_send.at[g, t], f_recv.at[g, z], me_t * 2 + x, t)

    def relay_copy(g, cc):
        return rcopy(tin.at[cc, span(g)], fin.at[z, span(g)], r_send.at[g, cc], f_recv.at[g, z], ((1 - y) * 2 + cc) * 2 + x, me_t)

    tile = 512

    def passed(g):
        @pl.when(is_inner)
        def _():
            for i in range(2):
                rcopy(
                    hid.at[span(g)], land.at[i, span(g)], a_send.at[g, 1], n_recv.at[g, i], landing(i) * 2 + x, me_t
                ).wait_recv()
                n_out(g, i).start()

                @pl.when(landing(i) != me_t)
                def _():
                    n_near(g, i).start()

                @pl.when(landing(i) == me_t)
                def _():
                    n_own(g, i).start()
                    hb[0, me_t, span(g)] = land[i, span(g)]

    def spread(g):
        @pl.when(home)
        def _():
            hb[0, me_t, span(g)] = hid[span(g)]

        for t in range(4):
            @pl.when(jnp.logical_not((home | landed) & (me_t == t)))
            def _():
                a_copy_in = rcopy(hid.at[span(g)], hb.at[0, t, span(g)], a_send.at[g, 0], a_recv.at[g, t], me_v, t)
                a_copy_in.wait_recv()
                x_copy(g, t).start()

    def logits_of(g):
        if g == 0:
            weights.wait()
        for t in range(4):
            x_copy(g, t).wait_recv()

        @pl.loop(0, width // tile)
        def _(j):
            cols = pl.ds(pl.multiple_of(j * tile, tile), tile)
            total = None
            for q in range(2):
                lhs = hb[q, :, span(g), :].reshape(4 * sizes[g], feats)
                term = jnp.dot(lhs, wbuf[weight_rows(q), cols], preferred_element_type=F32)
                total = term if total is None else total + term
            plog[:, span(g), cols] = total.reshape(4, sizes[g], tile)

        pair_copy(g, 1).start()
        pair_copy(g, 0).start()

    def cross_over(g):
        pair_copy(g, 1).wait_recv()
        value = plog[tok_of(2), span(g), :] + pin[1, span(g), :]
        top_of = jnp.max(jnp.abs(value), axis=1, keepdims=True)
        power = jnp.ceil(jnp.log2(jnp.maximum(top_of, jnp.float32(1e-20))) + jnp.float32(0.001))
        coded = jnp.round(value * jnp.exp2(15.0 - power)).astype(jnp.int32)
        xo[span(g), 0:width] = coded.astype(I16)
        xo[span(g), width:width + EXTRA] = jnp.broadcast_to(power.astype(jnp.int32), (sizes[g], EXTRA)).astype(I16)
        cross_copy(g).start()

    def softmax_of(g):
        pair_copy(g, 0).wait_recv()
        near_half = plog[me_t, span(g), :] + pin[0, span(g), :]
        cross_copy(g).wait_recv()
        power = xi[span(g), width:width + EXTRA].astype(jnp.int32).astype(F32)[:, 0:1]
        logits = near_half + xi[span(g), 0:width].astype(jnp.int32).astype(F32) * jnp.exp2(power - 15.0)
        masked = jnp.where(mask_ref[...] == 1, logits, jnp.float32(-1e30))
        local_max = jnp.max(masked, axis=1, keepdims=True)
        local_target = jnp.sum(jnp.where(onehot_of(g), logits, 0.0), axis=1, keepdims=True)
        local_sum = jnp.sum(jnp.exp(masked - local_max), axis=1, keepdims=True)
        m = sizes[g]
        lanes = lax.broadcasted_iota(jnp.int32, (m, 128), 1)
        packed = jnp.where(lanes == 0, local_max, jnp.where(lanes == 1, local_sum, local_target))
        if m < 128:
            packed = jnp.concatenate([packed, jnp.zeros((128 - m, 128), F32)], axis=0)
        mine = jnp.transpose(packed)[0:8]
        stats_out[g] = mine
        stats_in[g, me_v] = mine
        msk[span(g), :] = masked
        for k in range(1, nv):
            stat_copy(g, k).start()

    def grads_of(g):
        for k in range(1, nv):
            source = (me_v + nv - k) % nv
            rcopy(stats_out.at[g], stats_in.at[g, source], s_send.at[g, k], s_recv.at[g, source], source, me_t).wait_recv()
        row_max = stats_in[g, 0][0:1]
        for v in range(1, nv):
            row_max = jnp.maximum(row_max, stats_in[g, v][0:1])
        denominator = jnp.zeros_like(row_max)
        target_logit = jnp.zeros_like(row_max)
        for v in range(nv):
            got = stats_in[g, v]
            denominator += got[1:2] * jnp.exp(got[0:1] - row_max)
            target_logit += got[2:3]
        log_norm = row_max + jnp.log(denominator)
        loss_rows[g] = log_norm - target_logit
        column = jnp.transpose(jnp.broadcast_to(log_norm, (128, 128)))[0:sizes[g], 0:1]
        probabilities = jnp.exp(msk[span(g), :] - column)
        tok_grad = sides[firsts[g]:firsts[g] + sizes[g], 1:2]
        dl[me_t, span(g), :] = (tok_grad * (probabilities - onehot_of(g).astype(F32))).astype(BF)
        grad_copy(g, 0).start()
        grad_copy(g, 1).start()

    def grads_on(g):
        t = tok_of(2)
        rcopy(dl.at[t, span(g)], dl.at[t, span(g)], d_send.at[g, 0], d_recv.at[g, 0], me_v, t).wait_recv()
        grad_copy(g, 2).start()

    def terms_of(g):
        for i, r in ((1, 1), (2, 3)):
            t = tok_of(r)
            rcopy(dl.at[t, span(g)], dl.at[t, span(g)], d_send.at[g, i], d_recv.at[g, i], me_v, tok_of(1)).wait_recv()
        lhs = dl[:, span(g), :].reshape(4 * sizes[g], width)
        for q in (1, 0):
            value = lax.dot_general(
                lhs, wbuf[weight_rows(q), :], (((1,), (1,)), ((), ())), preferred_element_type=F32
            ).reshape(4, sizes[g], feats)
            if q == 0:
                near[:, span(g), :] = value
            else:
                mix_out[:, span(g), :] = value.astype(BF)
                for r in (2, 3, 1, 0):
                    mix_copy(g, tok_of(r)).start()

    def mixed(g, r):
        t = tok_of(r)
        mix_copy(g, t).wait_recv()
        both = (near[t, span(g), :] + mix_in[t, span(g), :].astype(F32)).astype(BF)
        if r == 0:
            @pl.when(home)
            def _():
                fin[z, span(g), :] = both

            @pl.when(jnp.logical_not(home))
            def _():
                eo[t, span(g), :] = both
                far_copy(g, t).start()
        elif r == 1:
            eo[t, span(g), :] = both
            far_copy(g, t).start()
        else:
            eo[t, span(g), :] = both

            @pl.when(home)
            def _():
                near_copy(g, t).start()

            @pl.when(jnp.logical_not(home))
            def _():
                pass_copy(g, t).start()

    def relayed(g, r):
        cc = (c + r) % 2

        @pl.when((1 - y) * 2 + cc != z)
        def _():
            rcopy(eo.at[0, span(g)], tin.at[cc, span(g)], e_send.at[g, 0], t_recv.at[g, cc], me_v, (1 - y) * 2 + cc).wait_recv()
            relay_copy(g, cc).start()

    def finish(g):
        total = None
        for zz in range(4):
            @pl.when(jnp.logical_not(home & (z == zz)))
            def _():
                rcopy(eo.at[0, span(g)], fin.at[zz, span(g)], e_send.at[g, 0], f_recv.at[g, zz], zz * 2 + x, me_t).wait_recv()
        for zz in range(4):
            term = fin[zz, span(g), :].astype(F32)
            total = term if total is None else total + term
        out_ref[span(g), :] = total.astype(BF)

    steps = {
        "ga": gather, "ld": passed, "sp": spread, "lg": logits_of, "co": cross_over, "sm": softmax_of, "gr": grads_of, "go": grads_on,
        "tm": terms_of, "fi": finish,
    }
    for r in range(4):
        steps[f"m{r}"] = lambda g, r=r: mixed(g, r)
    for r in range(2):
        steps[f"r{r}"] = lambda g, r=r: relayed(g, r)
    for item in PLAN:
        steps[item[:2]](int(item[2:]))

    loss_ref[...] = jnp.concatenate([loss_rows[g][:, 0:sizes[g]] for g in range(groups)], axis=1)

    for g in range(groups):
        a_copy(g).wait_send()
        n_copy(g).wait_send()

        @pl.when(jnp.logical_not(home))
        def _():
            o_copy(g).wait_send()

        @pl.when(is_inner)
        def _():
            for i in range(2):
                n_out(g, i).wait_send()

                @pl.when(landing(i) != me_t)
                def _():
                    n_near(g, i).wait_send()

        for t in range(4):
            x_copy(g, t).wait_send()
            mix_copy(g, t).wait_send()

            @pl.when(jnp.logical_not(home & (me_t == t)))
            def _():
                pass_copy(g, t).wait_send()

        for k in range(2):
            pair_copy(g, k).wait_send()

            @pl.when((1 - y) * 2 + k != z)
            def _():
                relay_copy(g, k).wait_send()

        cross_copy(g).wait_send()
        for k in range(1, nv):
            stat_copy(g, k).wait_send()
        for i in range(3):
            grad_copy(g, i).wait_send()


def fused(vocab_size, tok_size):
    def on_device(hidden, head_weight, targets, vocab_mask, token_grad):
        rows, feats = hidden.shape
        width = head_weight.shape[1]
        groups = len(SIZES)
        dma = pltpu.SemaphoreType.DMA
        vmem = pl.BlockSpec(memory_space=pltpu.VMEM)
        hbm = pl.BlockSpec(memory_space=pltpu.HBM)
        hidden_grad, loss = pl.pallas_call(
            lambda *refs: kernel(SIZES, *refs),
            out_shape=(
                jax.ShapeDtypeStruct((rows, feats), BF),
                jax.ShapeDtypeStruct((1, rows), F32),
            ),
            in_specs=[hbm, hbm] + [vmem] * 3,
            out_specs=(vmem, vmem),
            scratch_shapes=[
                pltpu.VMEM((rows, feats), BF),
                pltpu.VMEM((2 * feats, width), BF),
                pltpu.VMEM((2, rows, feats), BF),
                pltpu.VMEM((2, 4, rows, feats), BF),
                pltpu.VMEM((4, rows, width), F32),
                pltpu.VMEM((2, rows, width), F32),
                pltpu.VMEM((rows, width + EXTRA), I16),
                pltpu.VMEM((rows, width + EXTRA), I16),
                pltpu.VMEM((rows, width), F32),
                pltpu.VMEM((groups, 8, 128), F32),
                pltpu.VMEM((groups, vocab_size, 8, 128), F32),
                pltpu.VMEM((groups, 1, 128), F32),
                pltpu.VMEM((4, rows, width), BF),
                pltpu.VMEM((4, rows, feats), BF),
                pltpu.VMEM((4, rows, feats), BF),
                pltpu.VMEM((4, rows, feats), F32),
                pltpu.VMEM((4, rows, feats), BF),
                pltpu.VMEM((2, rows, feats), BF),
                pltpu.VMEM((4, rows, feats), BF),
                dma((groups,)), dma,
                dma((groups, 3)), dma((groups, 4)), dma((groups, 2)), dma((groups, 2, 2)), dma((groups, 4)), dma((groups, 4)),
                dma((groups, 2)), dma((groups, 2)), dma((groups,)), dma((groups,)),
                dma((groups, 8)), dma((groups, 8)), dma((groups, 3)), dma((groups, 3)),
                dma((groups, 4)), dma((groups, 4)), dma((groups, 4)), dma((groups, 4)),
                dma((groups, 2)), dma((groups, 2)),
            ],
            compiler_params=pltpu.CompilerParams(
                collective_id=0, has_side_effects=True, vmem_limit_bytes=60 * 1024 * 1024
            ),
        )(hidden, head_weight, targets[None, :], vocab_mask[None, :], token_grad[None, :])
        def hand_on(grad_ref, loss_ref, grad_out, loss_out, grad_buf, loss_buf, sem):
            ins = [
                pltpu.make_async_copy(loss_ref, loss_buf, sem.at[0]),
                pltpu.make_async_copy(grad_ref, grad_buf, sem.at[1]),
            ]
            outs = [
                pltpu.make_async_copy(loss_buf, loss_out, sem.at[2]),
                pltpu.make_async_copy(grad_buf, grad_out, sem.at[3]),
            ]
            for copy in ins:
                copy.start()
            for copy, after in zip(ins, outs):
                copy.wait()
                after.start()
            for copy in outs:
                copy.wait()

        hidden_grad, loss = pl.pallas_call(
            hand_on,
            out_shape=(
                jax.ShapeDtypeStruct((rows, feats), BF),
                jax.ShapeDtypeStruct((1, rows), F32),
            ),
            in_specs=[hbm, hbm],
            out_specs=(hbm, hbm),
            scratch_shapes=[pltpu.VMEM((rows, feats), BF), pltpu.VMEM((1, rows), F32), dma((4,))],
        )(hidden_grad, loss)
        return (hidden_grad, loss.reshape(rows))

    return on_device


def solution(mesh):
    placed = (P("tok", "vocab"), P("tok", "vocab"), P("tok"), P("vocab"), P("tok"))
    vocab_size, tok_size = mesh.shape["vocab"], mesh.shape["tok"]

    def body(hidden, head_weight, *rest):
        rows, feats = hidden.shape
        fits = tok_size == 4 and vocab_size == 8 and feats % 128 == 0 and head_weight.shape[1] % 256 == 0
        fits = fits and rows <= 256 and rows == sum(SIZES)
        build = fused if fits else make_on_device
        return build(vocab_size, tok_size)(hidden, head_weight, *rest)

    return jax.shard_map(
        body,
        mesh=mesh,
        in_specs=placed,
        out_specs=(P("tok", "vocab"), P("tok")),
        check_vma=False,
    )
```

```python
import jax
import jax.numpy as jnp
from jax import lax
from jax.experimental import pallas as pl
from jax.experimental.pallas import tpu as pltpu
from jax.sharding import PartitionSpec as P


def make_on_device(vocab_size, tok_size):
    share = vocab_size // tok_size
    moves = [
        (b * tok_size + a, (a * share + b % share) * tok_size + b // share)
        for a in range(tok_size)
        for b in range(vocab_size)
    ]
    back = [(there, here) for here, there in moves]

    def on_device(hidden, head_weight, targets, vocab_mask, token_grad):
        rows, feats = hidden.shape
        block_width = head_weight.shape[1]
        moved = lax.ppermute(hidden, ("vocab", "tok"), moves)
        pieces = lax.all_gather(moved, "vocab")
        gathered = (
            pieces.reshape(tok_size, share, rows, feats)
            .transpose(0, 2, 1, 3)
            .reshape(tok_size * rows, share * feats)
        )
        partial_logits = jnp.dot(gathered, head_weight, preferred_element_type=jnp.float32)
        logits = lax.psum_scatter(partial_logits, "tok", scatter_dimension=0, tiled=True)
        first_column = lax.axis_index("vocab") * block_width
        masked = jnp.where(vocab_mask[None, :] == 1, logits, jnp.float32(-1e30))
        local_max = jnp.max(masked, axis=1)
        columns = first_column + jnp.arange(block_width, dtype=jnp.int32)
        onehot = columns[None, :] == targets[:, None]
        local_target = jnp.sum(jnp.where(onehot, logits, jnp.float32(0.0)), axis=1)
        weights = jnp.exp(masked - local_max[:, None])
        local_sum = jnp.sum(weights, axis=1)
        stats = lax.all_gather(jnp.stack([local_max, local_sum, local_target]), "vocab")
        row_max = jnp.max(stats[:, 0], axis=0)
        denominator = jnp.sum(stats[:, 1] * jnp.exp(stats[:, 0] - row_max[None]), axis=0)
        target_logit = jnp.sum(stats[:, 2], axis=0)
        log_norm = row_max + jnp.log(denominator)
        token_loss = log_norm - target_logit
        probabilities = jnp.exp(masked - log_norm[:, None])
        logit_grad = (
            token_grad[:, None] * (probabilities - onehot.astype(jnp.float32))
        ).astype(jnp.bfloat16)
        all_grads = lax.all_gather(logit_grad, "tok", axis=0, tiled=True)
        partial_value = lax.dot_general(
            all_grads,
            head_weight,
            (((1,), (1,)), ((), ())),
            preferred_element_type=jnp.float32,
        )
        blocks = (
            partial_value.reshape(tok_size, rows, share, feats)
            .transpose(0, 2, 1, 3)
            .reshape(vocab_size, rows, feats)
        )
        summed = lax.psum_scatter(blocks, "vocab", scatter_dimension=0, tiled=False)
        hidden_grad = lax.ppermute(summed.astype(jnp.bfloat16), ("vocab", "tok"), back)
        return (hidden_grad, token_loss)

    return on_device


SIZES = (48, 48, 48, 48)
EXTRA = 128
BF = jnp.bfloat16
F32 = jnp.float32
I16 = jnp.int16


PLAN = (
    "ga0", "ld0", "ga1", "sp0", "ld1", "ga2", "sp1", "ld2", "lg0", "ga3", "co0", "sp2", "sm0", "ld3", "lg1",
    "co1", "sp3", "gr0", "lg2", "sm1", "co2", "go0", "tm0", "gr1", "lg3", "m20", "sm2", "go1", "co3", "m30",
    "r00", "tm1", "m10", "gr2", "sm3", "r10", "m21", "go2", "m00", "m31", "tm2", "m11", "r01", "gr3", "m01",
    "m22", "r11", "m32", "go3", "r02", "fi0", "tm3", "m12", "r12", "m23", "m02", "m33", "m13", "m03", "r03",
    "r13", "fi2", "fi1", "fi3",
)


def kernel(
    sizes,
    hidden_ref, weight_ref, targets_ref, mask_ref, grad_ref,
    out_ref, loss_ref,
    out_buf, loss_buf, o_sem, hid, wbuf, land, hb, plog, pin, xo, xi, msk, stats_out, stats_in, loss_rows, dl,
    mix_out, mix_in, near, eo, tin, fin,
    l_sem, w_sem, a_send, a_recv, n_recv, n_send, x_send, x_recv, p_send, p_recv, c_send, c_recv,
    s_send, s_recv, d_send, d_recv, m_send, m_recv, e_send, f_recv, t_recv, r_send,
):
    rows, feats = hidden_ref.shape
    groups = len(sizes)
    firsts = [sum(sizes[:g]) for g in range(groups)]
    width = weight_ref.shape[1]
    me_v = lax.axis_index("vocab")
    me_t = lax.axis_index("tok")
    z, x = me_v // 2, me_v % 2
    y, c = me_t // 2, me_t % 2
    nv = 8

    def dev(v, t):
        return {"vocab": v, "tok": t}

    def tok_of(r):
        return ((y + r // 2) % 2) * 2 + (c + r % 2) % 2

    other_x = z * 2 + (1 - x)

    def rcopy(src, dst, ss, rs, v, t):
        return pltpu.make_async_remote_copy(
            src_ref=src, dst_ref=dst, send_sem=ss, recv_sem=rs,
            device_id=dev(v, t), device_id_type=pl.DeviceIdType.MESH,
        )

    def span(g):
        return pl.ds(firsts[g], sizes[g])

    loads = [pltpu.make_async_copy(hidden_ref.at[span(g)], hid.at[span(g)], l_sem.at[g]) for g in range(groups)]
    for load in loads:
        load.start()
    weights = pltpu.make_async_copy(weight_ref, wbuf, w_sem)
    weights.start()

    barrier = pltpu.get_barrier_semaphore()
    for k in range(4):
        for r in range(4):
            if k or r:
                pl.semaphore_signal(
                    barrier, inc=1, device_id=dev(((z + k) % 4) * 2 + x, tok_of(r)), device_id_type=pl.DeviceIdType.MESH
                )
        pl.semaphore_signal(
            barrier, inc=1, device_id=dev(((z + k) % 4) * 2 + 1 - x, me_t), device_id_type=pl.DeviceIdType.MESH
        )
    pl.semaphore_wait(barrier, 19)

    home = me_t == z

    side = z // 2
    partner = z + 1 - 2 * (z % 2)
    inner = jnp.where(z < 2, 2, 1)
    outer = jnp.where(z < 2, 0, 3)
    is_inner = (z == 1) | (z == 2)
    landed = is_inner & (me_t // 2 == 1 - side)

    def a_copy(g):
        return rcopy(hid.at[span(g)], hb.at[0, me_t, span(g)], a_send.at[g, 0], a_recv.at[g, me_t], partner * 2 + x, z)

    def n_copy(g):
        i = jnp.where(is_inner, 0, 1)
        return rcopy(hid.at[span(g)], land.at[i, span(g)], a_send.at[g, 1], n_recv.at[g, i], inner * 2 + x, me_t)

    def o_copy(g):
        return rcopy(hid.at[span(g)], hb.at[0, me_t, span(g)], a_send.at[g, 2], a_recv.at[g, me_t], me_v, z)

    def landing(i):
        return jnp.where(z == 2, 1 - i, 2 + i)

    def n_out(g, i):
        return rcopy(
            land.at[i, span(g)], hb.at[0, me_t, span(g)], n_send.at[g, i, 0], a_recv.at[g, me_t], outer * 2 + x, landing(i)
        )

    def n_near(g, i):
        return rcopy(land.at[i, span(g)], hb.at[0, me_t, span(g)], n_send.at[g, i, 1], a_recv.at[g, me_t], me_v, landing(i))

    def n_own(g, i):
        return rcopy(land.at[i, span(g)], hb.at[1, me_t, span(g)], x_send.at[g, me_t], x_recv.at[g, me_t], other_x, me_t)

    def x_copy(g, t):
        return rcopy(hb.at[0, t, span(g)], hb.at[1, t, span(g)], x_send.at[g, t], x_recv.at[g, t], other_x, me_t)

    def x_own(g):
        return rcopy(hid.at[span(g)], hb.at[1, me_t, span(g)], x_send.at[g, me_t], x_recv.at[g, me_t], other_x, me_t)

    def gather(g):
        loads[g].wait()
        a_copy(g).start()
        n_copy(g).start()

        @pl.when(jnp.logical_not(home))
        def _():
            o_copy(g).start()

        @pl.when(home)
        def _():
            x_own(g).start()


    top = jnp.concatenate([targets_ref[...].astype(F32), grad_ref[...]], axis=0)
    top = jnp.concatenate([top, jnp.zeros((2, 256 - rows), F32)], axis=1)
    sides = jnp.transpose(jnp.concatenate([top, jnp.zeros((126, 256), F32)], axis=0))

    def onehot_of(g):
        columns = me_v * width + lax.broadcasted_iota(jnp.int32, (sizes[g], width), 1)
        return columns == sides[firsts[g]:firsts[g] + sizes[g], 0:1].astype(jnp.int32)

    def weight_rows(q):
        owner = (x + q) % 2
        return pl.ds(pl.multiple_of(owner * feats, 128), feats)

    def pair_copy(g, k):
        return rcopy(plog.at[tok_of(1 + 2 * k), span(g)], pin.at[k, span(g)], p_send.at[g, k], p_recv.at[g, k], me_v, tok_of(1))

    def cross_copy(g):
        return rcopy(xo.at[span(g)], xi.at[span(g)], c_send.at[g], c_recv.at[g], me_v, tok_of(2))

    def stat_copy(g, k):
        return rcopy(stats_out.at[g], stats_in.at[g, me_v], s_send.at[g, k], s_recv.at[g, me_v], (me_v + k) % nv, me_t)

    def grad_copy(g, i):
        t = tok_of(2) if i == 2 else me_t
        return rcopy(dl.at[t, span(g)], dl.at[t, span(g)], d_send.at[g, i], d_recv.at[g, i], me_v, tok_of(2 if i == 0 else 1))

    def mix_copy(g, t):
        return rcopy(mix_out.at[t, span(g)], mix_in.at[t, span(g)], m_send.at[g, t], m_recv.at[g, t], other_x, me_t)

    def pass_copy(g, t):
        return rcopy(eo.at[t, span(g)], tin.at[c, span(g)], e_send.at[g, t], t_recv.at[g, c], me_v, t)

    def near_copy(g, t):
        return rcopy(eo.at[t, span(g)], fin.at[z, span(g)], e_send.at[g, t], f_recv.at[g, z], me_v, t)

    def far_copy(g, t):
        return rcopy(eo.at[t, span(g)], fin.at[z, span(g)], e_send.at[g, t], f_recv.at[g, z], me_t * 2 + x, t)

    def relay_copy(g, cc):
        return rcopy(tin.at[cc, span(g)], fin.at[z, span(g)], r_send.at[g, cc], f_recv.at[g, z], ((1 - y) * 2 + cc) * 2 + x, me_t)

    tile = 512

    def passed(g):
        @pl.when(is_inner)
        def _():
            for i in range(2):
                rcopy(
                    hid.at[span(g)], land.at[i, span(g)], a_send.at[g, 1], n_recv.at[g, i], landing(i) * 2 + x, me_t
                ).wait_recv()
                n_out(g, i).start()

                @pl.when(landing(i) != me_t)
                def _():
                    n_near(g, i).start()

                @pl.when(landing(i) == me_t)
                def _():
                    n_own(g, i).start()
                    hb[0, me_t, span(g)] = land[i, span(g)]

    def spread(g):
        @pl.when(home)
        def _():
            hb[0, me_t, span(g)] = hid[span(g)]

        for t in range(4):
            @pl.when(jnp.logical_not((home | landed) & (me_t == t)))
            def _():
                a_copy_in = rcopy(hid.at[span(g)], hb.at[0, t, span(g)], a_send.at[g, 0], a_recv.at[g, t], me_v, t)
                a_copy_in.wait_recv()
                x_copy(g, t).start()

    def logits_of(g):
        if g == 0:
            weights.wait()
        for t in range(4):
            x_copy(g, t).wait_recv()

        @pl.loop(0, width // tile)
        def _(j):
            cols = pl.ds(pl.multiple_of(j * tile, tile), tile)
            total = None
            for q in range(2):
                lhs = hb[q, :, span(g), :].reshape(4 * sizes[g], feats)
                term = jnp.dot(lhs, wbuf[weight_rows(q), cols], preferred_element_type=F32)
                total = term if total is None else total + term
            plog[:, span(g), cols] = total.reshape(4, sizes[g], tile)

        pair_copy(g, 1).start()
        pair_copy(g, 0).start()

    def cross_over(g):
        pair_copy(g, 1).wait_recv()
        value = plog[tok_of(2), span(g), :] + pin[1, span(g), :]
        top_of = jnp.max(jnp.abs(value), axis=1, keepdims=True)
        power = jnp.ceil(jnp.log2(jnp.maximum(top_of, jnp.float32(1e-20))) + jnp.float32(0.001))
        coded = jnp.round(value * jnp.exp2(15.0 - power)).astype(jnp.int32)
        xo[span(g), 0:width] = coded.astype(I16)
        xo[span(g), width:width + EXTRA] = jnp.broadcast_to(power.astype(jnp.int32), (sizes[g], EXTRA)).astype(I16)
        cross_copy(g).start()

    def softmax_of(g):
        pair_copy(g, 0).wait_recv()
        near_half = plog[me_t, span(g), :] + pin[0, span(g), :]
        cross_copy(g).wait_recv()
        power = xi[span(g), width:width + EXTRA].astype(jnp.int32).astype(F32)[:, 0:1]
        logits = near_half + xi[span(g), 0:width].astype(jnp.int32).astype(F32) * jnp.exp2(power - 15.0)
        masked = jnp.where(mask_ref[...] == 1, logits, jnp.float32(-1e30))
        local_max = jnp.max(masked, axis=1, keepdims=True)
        local_target = jnp.sum(jnp.where(onehot_of(g), logits, 0.0), axis=1, keepdims=True)
        local_sum = jnp.sum(jnp.exp(masked - local_max), axis=1, keepdims=True)
        m = sizes[g]
        lanes = lax.broadcasted_iota(jnp.int32, (m, 128), 1)
        packed = jnp.where(lanes == 0, local_max, jnp.where(lanes == 1, local_sum, local_target))
        if m < 128:
            packed = jnp.concatenate([packed, jnp.zeros((128 - m, 128), F32)], axis=0)
        mine = jnp.transpose(packed)[0:8]
        stats_out[g] = mine
        stats_in[g, me_v] = mine
        msk[span(g), :] = masked
        for k in range(1, nv):
            stat_copy(g, k).start()

    def grads_of(g):
        for k in range(1, nv):
            source = (me_v + nv - k) % nv
            rcopy(stats_out.at[g], stats_in.at[g, source], s_send.at[g, k], s_recv.at[g, source], source, me_t).wait_recv()
        row_max = stats_in[g, 0][0:1]
        for v in range(1, nv):
            row_max = jnp.maximum(row_max, stats_in[g, v][0:1])
        denominator = jnp.zeros_like(row_max)
        target_logit = jnp.zeros_like(row_max)
        for v in range(nv):
            got = stats_in[g, v]
            denominator += got[1:2] * jnp.exp(got[0:1] - row_max)
            target_logit += got[2:3]
        log_norm = row_max + jnp.log(denominator)
        loss_rows[g] = log_norm - target_logit
        column = jnp.transpose(jnp.broadcast_to(log_norm, (128, 128)))[0:sizes[g], 0:1]
        probabilities = jnp.exp(msk[span(g), :] - column)
        tok_grad = sides[firsts[g]:firsts[g] + sizes[g], 1:2]
        dl[me_t, span(g), :] = (tok_grad * (probabilities - onehot_of(g).astype(F32))).astype(BF)
        grad_copy(g, 0).start()
        grad_copy(g, 1).start()

    def grads_on(g):
        t = tok_of(2)
        rcopy(dl.at[t, span(g)], dl.at[t, span(g)], d_send.at[g, 0], d_recv.at[g, 0], me_v, t).wait_recv()
        grad_copy(g, 2).start()

    def terms_of(g):
        for i, r in ((1, 1), (2, 3)):
            t = tok_of(r)
            rcopy(dl.at[t, span(g)], dl.at[t, span(g)], d_send.at[g, i], d_recv.at[g, i], me_v, tok_of(1)).wait_recv()
        lhs = dl[:, span(g), :].reshape(4 * sizes[g], width)
        for q in (1, 0):
            value = lax.dot_general(
                lhs, wbuf[weight_rows(q), :], (((1,), (1,)), ((), ())), preferred_element_type=F32
            ).reshape(4, sizes[g], feats)
            if q == 0:
                near[:, span(g), :] = value
            else:
                mix_out[:, span(g), :] = value.astype(BF)
                for r in (2, 3, 1, 0):
                    mix_copy(g, tok_of(r)).start()

    def mixed(g, r):
        t = tok_of(r)
        mix_copy(g, t).wait_recv()
        both = (near[t, span(g), :] + mix_in[t, span(g), :].astype(F32)).astype(BF)
        if r == 0:
            @pl.when(home)
            def _():
                fin[z, span(g), :] = both

            @pl.when(jnp.logical_not(home))
            def _():
                eo[t, span(g), :] = both
                far_copy(g, t).start()
        elif r == 1:
            eo[t, span(g), :] = both
            far_copy(g, t).start()
        else:
            eo[t, span(g), :] = both

            @pl.when(home)
            def _():
                near_copy(g, t).start()

            @pl.when(jnp.logical_not(home))
            def _():
                pass_copy(g, t).start()

    def relayed(g, r):
        cc = (c + r) % 2

        @pl.when((1 - y) * 2 + cc != z)
        def _():
            rcopy(eo.at[0, span(g)], tin.at[cc, span(g)], e_send.at[g, 0], t_recv.at[g, cc], me_v, (1 - y) * 2 + cc).wait_recv()
            relay_copy(g, cc).start()

    def out_copy(g):
        return pltpu.make_async_copy(out_buf.at[span(g)], out_ref.at[span(g)], o_sem.at[g])

    loss_copy = pltpu.make_async_copy(loss_buf, loss_ref, o_sem.at[groups])

    def finish(g):
        total = None
        for zz in range(4):
            @pl.when(jnp.logical_not(home & (z == zz)))
            def _():
                rcopy(eo.at[0, span(g)], fin.at[zz, span(g)], e_send.at[g, 0], f_recv.at[g, zz], zz * 2 + x, me_t).wait_recv()
        for zz in range(4):
            term = fin[zz, span(g), :].astype(F32)
            total = term if total is None else total + term
        out_buf[span(g), :] = total.astype(BF)
        out_copy(g).start()

    steps = {
        "ga": gather, "ld": passed, "sp": spread, "lg": logits_of, "co": cross_over, "sm": softmax_of, "gr": grads_of, "go": grads_on,
        "tm": terms_of, "fi": finish,
    }
    for r in range(4):
        steps[f"m{r}"] = lambda g, r=r: mixed(g, r)
    for r in range(2):
        steps[f"r{r}"] = lambda g, r=r: relayed(g, r)
    pending = set(range(groups))
    for item in PLAN:
        steps[item[:2]](int(item[2:]))
        if item[:2] == "gr":
            pending.remove(int(item[2:]))
            if not pending:
                loss_buf[...] = jnp.concatenate([loss_rows[g][:, 0:sizes[g]] for g in range(groups)], axis=1)
                loss_copy.start()

    for g in range(groups):
        a_copy(g).wait_send()
        n_copy(g).wait_send()

        @pl.when(jnp.logical_not(home))
        def _():
            o_copy(g).wait_send()

        @pl.when(is_inner)
        def _():
            for i in range(2):
                n_out(g, i).wait_send()

                @pl.when(landing(i) != me_t)
                def _():
                    n_near(g, i).wait_send()

        for t in range(4):
            x_copy(g, t).wait_send()
            mix_copy(g, t).wait_send()

            @pl.when(jnp.logical_not(home & (me_t == t)))
            def _():
                pass_copy(g, t).wait_send()

        for k in range(2):
            pair_copy(g, k).wait_send()

            @pl.when((1 - y) * 2 + k != z)
            def _():
                relay_copy(g, k).wait_send()

        cross_copy(g).wait_send()
        for k in range(1, nv):
            stat_copy(g, k).wait_send()
        for i in range(3):
            grad_copy(g, i).wait_send()
        out_copy(g).wait()
    loss_copy.wait()


def fused(vocab_size, tok_size):
    def on_device(hidden, head_weight, targets, vocab_mask, token_grad):
        rows, feats = hidden.shape
        width = head_weight.shape[1]
        groups = len(SIZES)
        dma = pltpu.SemaphoreType.DMA
        vmem = pl.BlockSpec(memory_space=pltpu.VMEM)
        hbm = pl.BlockSpec(memory_space=pltpu.HBM)
        hidden_grad, loss = pl.pallas_call(
            lambda *refs: kernel(SIZES, *refs),
            out_shape=(
                jax.ShapeDtypeStruct((rows, feats), BF),
                jax.ShapeDtypeStruct((1, rows), F32),
            ),
            in_specs=[hbm, hbm] + [vmem] * 3,
            out_specs=(hbm, hbm),
            scratch_shapes=[
                pltpu.VMEM((rows, feats), BF),
                pltpu.VMEM((1, rows), F32),
                dma((groups + 1,)),
                pltpu.VMEM((rows, feats), BF),
                pltpu.VMEM((2 * feats, width), BF),
                pltpu.VMEM((2, rows, feats), BF),
                pltpu.VMEM((2, 4, rows, feats), BF),
                pltpu.VMEM((4, rows, width), F32),
                pltpu.VMEM((2, rows, width), F32),
                pltpu.VMEM((rows, width + EXTRA), I16),
                pltpu.VMEM((rows, width + EXTRA), I16),
                pltpu.VMEM((rows, width), F32),
                pltpu.VMEM((groups, 8, 128), F32),
                pltpu.VMEM((groups, vocab_size, 8, 128), F32),
                pltpu.VMEM((groups, 1, 128), F32),
                pltpu.VMEM((4, rows, width), BF),
                pltpu.VMEM((4, rows, feats), BF),
                pltpu.VMEM((4, rows, feats), BF),
                pltpu.VMEM((4, rows, feats), F32),
                pltpu.VMEM((4, rows, feats), BF),
                pltpu.VMEM((2, rows, feats), BF),
                pltpu.VMEM((4, rows, feats), BF),
                dma((groups,)), dma,
                dma((groups, 3)), dma((groups, 4)), dma((groups, 2)), dma((groups, 2, 2)), dma((groups, 4)), dma((groups, 4)),
                dma((groups, 2)), dma((groups, 2)), dma((groups,)), dma((groups,)),
                dma((groups, 8)), dma((groups, 8)), dma((groups, 3)), dma((groups, 3)),
                dma((groups, 4)), dma((groups, 4)), dma((groups, 4)), dma((groups, 4)),
                dma((groups, 2)), dma((groups, 2)),
            ],
            compiler_params=pltpu.CompilerParams(
                collective_id=0, has_side_effects=True, vmem_limit_bytes=60 * 1024 * 1024
            ),
        )(hidden, head_weight, targets[None, :], vocab_mask[None, :], token_grad[None, :])
        def hand_on(grad_ref, loss_ref, grad_out, loss_out, grad_buf, loss_buf, sem):
            ins = [
                pltpu.make_async_copy(loss_ref, loss_buf, sem.at[0]),
                pltpu.make_async_copy(grad_ref, grad_buf, sem.at[1]),
            ]
            outs = [
                pltpu.make_async_copy(loss_buf, loss_out, sem.at[2]),
                pltpu.make_async_copy(grad_buf, grad_out, sem.at[3]),
            ]
            for copy in ins:
                copy.start()
            for copy, after in zip(ins, outs):
                copy.wait()
                after.start()
            for copy in outs:
                copy.wait()

        hidden_grad, loss = pl.pallas_call(
            hand_on,
            out_shape=(
                jax.ShapeDtypeStruct((rows, feats), BF),
                jax.ShapeDtypeStruct((1, rows), F32),
            ),
            in_specs=[hbm, hbm],
            out_specs=(hbm, hbm),
            scratch_shapes=[pltpu.VMEM((rows, feats), BF), pltpu.VMEM((1, rows), F32), dma((4,))],
        )(hidden_grad, loss)
        return (hidden_grad, loss.reshape(rows))

    return on_device


def solution(mesh):
    placed = (P("tok", "vocab"), P("tok", "vocab"), P("tok"), P("vocab"), P("tok"))
    vocab_size, tok_size = mesh.shape["vocab"], mesh.shape["tok"]

    def body(hidden, head_weight, *rest):
        rows, feats = hidden.shape
        fits = tok_size == 4 and vocab_size == 8 and feats % 128 == 0 and head_weight.shape[1] % 256 == 0
        fits = fits and rows <= 256 and rows == sum(SIZES)
        build = fused if fits else make_on_device
        return build(vocab_size, tok_size)(hidden, head_weight, *rest)

    return jax.shard_map(
        body,
        mesh=mesh,
        in_specs=placed,
        out_specs=(P("tok", "vocab"), P("tok")),
        check_vma=False,
    )
```
